256 devices in a mesh: grp: 8 (over z_lo, core), tab: 32 (over x, z_hi, y).
Axes of the slice: x: 4, y: 4, z: 8 (z_hi: 2, z_lo: 4; z = z_hi * 4 + z_lo), core: 2. Of those that a mesh axis runs over, the one named last changes fastest.
Arguments:
- sample_ids: int32 [4, 8192, 2048], P(None, ('grp', 'tab')), may hold values from 0 to 1535
- id_weights: bfloat16 [4, 8192, 2048], P(None, ('grp', 'tab')), may hold values from 0.25 to 2
- dense_features: bfloat16 [4, 8192, 128], P(None, ('grp', 'tab')), may hold values from -6 to 6
- click_labels: int32 [4, 8192], P(None, ('grp', 'tab')), may hold values 0 or 1
- table_shards: bfloat16 [256, 1536, 128], P('tab'), may hold values from -1.1953125 to 1.1953125
- slot_table: int32 [256], replicated, may hold values from 0 to 255, each once
- top_weight: bfloat16 [256, 1024], replicated, may hold values from -0.375 to 0.375
- top_bias: float32 [1024], replicated, may hold values from -3 to 3
- out_weight: bfloat16 [1024], replicated, may hold values from -0.1875 to 0.1875
Outputs:
- logits: float32 [4, 8192], P(None, ('grp', 'tab'))
- grad_top: float32 [256, 1024], replicated
- grad_bias: float32 [1024], replicated
The draws below stay inside these ranges and needn't reach their ends.
Inputs may be any that keep to these rules, and one draw needn't show every extreme that they name: `slot_table`: a permutation: each table stands in exactly one slot.
All inputs are finite; a program needn't handle non-finite values. No bound on the sum of `click_labels` on one device may be relied on, other than what follows from the above.
Results may differ from the reference program's by a relative error of at most 0.0056.
Values may be sent and summed in bfloat16 or wider, within the bound.
A program may use at most 128 MiB of HBM per device.

```python
import math
import jax
import jax.numpy as jnp
import numpy as np
from jax import lax

DIM = 128
VOCAB = 1536
HIDDEN_SIZE = 1024
HOTS = 8
MB = 4
TABLES = 256
BATCH = 8192


def place_ends(entries, key, smallest, largest):
    dims = entries.shape
    spot = [jax.random.randint(jax.random.fold_in(key, axis), (), 0, dims[axis]) for axis in range(len(dims))]
    entries = entries.at[tuple(spot)].set(smallest)
    longest = dims.index(max(dims))
    spot[longest] = (spot[longest] + 1) % dims[longest]
    return entries.at[tuple(spot)].set(largest)


def shard_levels(stream_key, dims, cuts, low, high):
    level, own = 1.0, jax.random.fold_in(stream_key, 6)
    for dim, blocks in cuts:
        steps = jnp.exp(jax.random.uniform(jax.random.fold_in(own, dim), (blocks,), jnp.float32, low / len(cuts), high / len(cuts)))
        level = level * jnp.repeat(steps, dims[dim] // blocks).reshape([-1 if axis == dim else 1 for axis in range(len(dims))])
    return level


def cumulative_ranks(count, lean):
    weights = [(1 << 20) // math.isqrt(standing ** lean) + 1 for standing in range(1, count + 1)]
    spread = 1 + sum(weights) // (1 << 30)
    return np.cumsum(np.array([max(1, weight // spread) for weight in weights]))


def skewed_ids(own_key, shape, number_of, skew):
    table = cumulative_ranks(number_of, skew)
    pick = jax.random.randint(jax.random.fold_in(own_key, 1), shape, 0, int(table[number_of - 1]))
    standing = jnp.searchsorted(jnp.asarray(table, jnp.int32), pick, side="right")
    return jax.random.permutation(jax.random.fold_in(own_key, 2), number_of)[standing].astype(jnp.int32)


def bell_draw(own_key, dims, width, bound, shards=(), kind=jnp.bfloat16):
    drawn = jax.random.normal(own_key, dims, jnp.float32) * width
    if len(shards) > 0:
        drawn = shard_levels(own_key, dims, shards, -0.22, 0.18) * drawn
    return jnp.clip(drawn, min=-bound, max=bound).astype(kind)


def setup_inputs(seed: int = 0) -> dict:
    key_list = jax.random.split(jax.random.key(seed), 10)
    return {
        "sample_ids": place_ends(skewed_ids(key_list[0], (MB, BATCH, TABLES * HOTS), VOCAB, 2), jax.random.fold_in(key_list[0], 3), 0, VOCAB - 1).astype(jnp.int32),
        "id_weights": jnp.clip(0.25 + 1.75 * jax.random.uniform(key_list[1], (MB, BATCH, TABLES * HOTS), jnp.float32) ** shard_levels(key_list[1], (MB, BATCH, TABLES * HOTS), ((1, 256),), -0.2, 0.2), 0.25, 2.0).astype(jnp.bfloat16),
        "dense_features": bell_draw(key_list[2], (MB, BATCH, DIM), 1.0, 6.0, ((1, 256),)),
        "click_labels": place_ends((jax.random.randint(key_list[3], (MB, BATCH), 0, 2) < 1).astype(jnp.int32), jax.random.fold_in(key_list[3], 1), 0, 1),
        "table_shards": bell_draw(key_list[4], (TABLES, VOCAB, DIM), 0.2, 1.1953125, ((0, 32),)),
        "slot_table": jax.random.permutation(key_list[5], TABLES).astype(jnp.int32),
        "top_weight": bell_draw(key_list[6], (TABLES, HIDDEN_SIZE), TABLES ** -0.5, 0.375),
        "top_bias": bell_draw(key_list[7], (HIDDEN_SIZE,), 0.5, 3.0, (), jnp.float32),
        "out_weight": bell_draw(key_list[8], (HIDDEN_SIZE,), HIDDEN_SIZE ** -0.5, 0.1875),
    }


loss_scale = 32768.0

def reference(sample_ids, id_weights, dense_features, click_labels, table_shards, slot_table, top_weight, top_bias, out_weight):
    count = MB * BATCH
    ids_all = sample_ids.reshape(count, TABLES, HOTS)
    weights_all = id_weights.reshape(count, TABLES, HOTS).astype(jnp.float32)
    features = dense_features.reshape(count, DIM).astype(jnp.float32)
    earlier = jnp.arange(HOTS)[None, :] < jnp.arange(HOTS)[:, None]
    scale = 1.0 / jnp.sqrt(jnp.float32(DIM))

    def slot_scores(slot):
        table = slot_table[slot]
        slot_ids = lax.dynamic_index_in_dim(ids_all, table, axis=1, keepdims=False)
        slot_weights = lax.dynamic_index_in_dim(weights_all, table, axis=1, keepdims=False)
        same = slot_ids[:, :, None] == slot_ids[:, None, :]
        summed = lax.optimization_barrier(jnp.sum(jnp.where(same, slot_weights[:, None, :], jnp.float32(0.0)), axis=2))
        first = jnp.logical_not(jnp.any(same & earlier[None], axis=2))
        rounded = lax.optimization_barrier(summed.astype(jnp.bfloat16)).astype(jnp.float32)
        merged = jnp.where(first, rounded, jnp.float32(0.0))
        shard = lax.dynamic_index_in_dim(table_shards, slot, axis=0, keepdims=False)
        rows = shard[slot_ids].astype(jnp.float32)
        pooled = jnp.einsum('nh,nhe->ne', merged, rows).astype(jnp.bfloat16)
        pooled_wide = lax.optimization_barrier(pooled).astype(jnp.float32)
        return (lax.optimization_barrier(jnp.sum(pooled_wide * features, axis=1)) * scale).astype(jnp.bfloat16)
    scores = lax.map(slot_scores, jnp.arange(TABLES, dtype=jnp.int32)).T
    slot_weight = top_weight[slot_table]
    pre = jnp.dot(scores, slot_weight, preferred_element_type=jnp.float32) + top_bias
    gate = jax.nn.sigmoid(pre)
    hidden = (pre * gate).astype(jnp.bfloat16)
    logit_all = jnp.dot(hidden, out_weight, preferred_element_type=jnp.float32)
    labels = click_labels.reshape(count).astype(jnp.float32)
    delta = (jax.nn.sigmoid(logit_all) - labels) * (loss_scale / count)
    slope = gate * (1.0 + pre * (1.0 - gate))
    hidden_grad = (delta[:, None] * out_weight.astype(jnp.float32)[None, :] * slope).astype(jnp.bfloat16)
    hidden_grad = lax.optimization_barrier(hidden_grad)
    grad_slot = jnp.dot(scores.T, hidden_grad, preferred_element_type=jnp.float32)
    grad_bias = lax.optimization_barrier(jnp.sum(hidden_grad.astype(jnp.float32), axis=0))
    grad_top = jnp.zeros_like(grad_slot).at[slot_table].set(grad_slot)
    return (logit_all.reshape(MB, BATCH), grad_top, grad_bias)
```

```python
import functools
import math

import jax
import jax.numpy as jnp
from jax import lax
from jax.experimental import pallas as pl
from jax.experimental.pallas import tpu as pltpu
from jax.sharding import PartitionSpec as P

HOTS = 8
LANES = 128
MESH = pl.DeviceIdType.MESH
loss_scale = 32768.0

Z_BIT = 4
PLANE = 16
ROWS = 128


def place():
    grp, tab = lax.axis_index("grp"), lax.axis_index("tab")
    return grp, tab


def mirrored(grp):
    return (3 - grp // 2) * 2 + grp % 2


def order(step):
    return (step // 8) * 8 + (step % 2) * Z_BIT + (step // 2) % 4


def flip(value, offset, bits):
    total = 0
    for bit in range(bits):
        unit = 1 << bit
        one, two = (value // unit) % 2, (offset // unit) % 2
        total = total + (one + two - 2 * one * two) * unit
    return total


def peer_of(grp, tab, offset):
    cross = (offset // Z_BIT) % 2
    there = cross * mirrored(grp) + (1 - cross) * grp
    return {"grp": there, "tab": flip(tab, offset, 5)}


def gather_rows(source, index):
    dims = lax.GatherDimensionNumbers(
        offset_dims=(),
        collapsed_slice_dims=(0,),
        start_index_map=(0,),
        operand_batching_dims=(1,),
        start_indices_batching_dims=(1,),
    )
    return lax.gather(
        source, index[..., None], dims, slice_sizes=(1, 1),
        mode=lax.GatherScatterMode.PROMISE_IN_BOUNDS,
    )


def exchange_kernel(
    slots_ref, ids_hbm, weights_hbm, features_hbm, tables_hbm, scores_ref,
    ids_ref, weights_ref, features_ref, tables_ref, ids_t, weights_t, send, recv, feats, back, summed,
    load_sem, send_sem, recv_sem, fsend_sem, frecv_sem, bsend_sem, brecv_sem,
):
    grp, tab = place()
    peers = send.shape[0]
    own_slots, vocab, width = tables_ref.shape
    lines = own_slots * HOTS
    loads = [
        pltpu.make_async_copy(source, target, load_sem.at[at])
        for at, (source, target) in enumerate(
            [(features_hbm, features_ref), (ids_hbm, ids_ref), (weights_hbm, weights_ref), (tables_hbm, tables_ref)]
        )
    ]
    for load in loads:
        load.start()
    barrier = pltpu.get_barrier_semaphore()

    def greet(offset, _):
        pl.semaphore_signal(barrier, inc=1, device_id=peer_of(grp, tab, offset), device_id_type=MESH)
        return 0

    lax.fori_loop(1, peers, greet, 0)
    loads[0].wait()
    feats[0] = features_ref[...]
    loads[1].wait()
    loads[2].wait()
    per_block = LANES // HOTS
    for at in range(ids_ref.shape[1] // LANES):
        columns = slice(at * LANES, (at + 1) * LANES)
        held = slice(at * per_block, (at + 1) * per_block)
        ids = ids_ref[:, columns]
        code = jnp.left_shift((ids & 127) + 128, jnp.right_shift(ids, 7))
        ids_t[held] = code.astype(jnp.float32).T.reshape(per_block, HOTS, LANES)
        weights_t[held] = weights_ref[:, columns].astype(jnp.float32).T.reshape(per_block, HOTS, LANES)

    def packed(offset, target):
        first = flip(tab, offset, 5) * own_slots
        for pair in range(own_slots // 2):
            one, two = slots_ref[first + 2 * pair], slots_ref[first + 2 * pair + 1]
            rows = slice(pair * 2 * HOTS, (pair + 1) * 2 * HOTS)
            target[offset, rows, :] = jnp.concatenate([ids_t[one], ids_t[two]], axis=0).astype(jnp.bfloat16)
            rows = slice(lines + pair * 2 * HOTS, lines + (pair + 1) * 2 * HOTS)
            target[offset, rows, :] = jnp.concatenate([weights_t[one], weights_t[two]], axis=0).astype(jnp.bfloat16)

    packed(0, recv)
    pl.semaphore_wait(barrier, peers - 1)

    def feature_copy(source, offset):
        return pltpu.make_async_remote_copy(
            src_ref=source, dst_ref=feats.at[offset],
            send_sem=fsend_sem.at[offset], recv_sem=frecv_sem.at[offset],
            device_id=peer_of(grp, tab, offset), device_id_type=MESH,
        )

    def passed_on(offset):
        return pltpu.make_async_remote_copy(
            src_ref=feats.at[Z_BIT], dst_ref=feats.at[offset + Z_BIT],
            send_sem=fsend_sem.at[offset + Z_BIT], recv_sem=frecv_sem.at[offset + Z_BIT],
            device_id=peer_of(grp, tab, offset), device_id_type=MESH,
        )

    def payload_copy(offset):
        return pltpu.make_async_remote_copy(
            src_ref=send.at[offset], dst_ref=recv.at[offset],
            send_sem=send_sem.at[offset], recv_sem=recv_sem.at[offset],
            device_id=peer_of(grp, tab, offset), device_id_type=MESH,
        )

    def score_copy(offset):
        return pltpu.make_async_remote_copy(
            src_ref=back.at[offset], dst_ref=scores_ref.at[tab],
            send_sem=bsend_sem.at[offset], recv_sem=brecv_sem.at[offset],
            device_id=peer_of(grp, tab, offset), device_id_type=MESH,
        )

    feature_copy(features_ref, Z_BIT).start()

    def send_features(m, _):
        feature_copy(features_ref, order(2 * m)).start()
        return 0

    lax.fori_loop(1, PLANE, send_features, 0)


    def send_payload(step, _):
        offset = order(step)
        packed(offset, send)
        payload_copy(offset).start()
        return 0

    lax.fori_loop(1, peers, send_payload, 0)
    feature_copy(features_ref, Z_BIT).wait_recv()

    def pass_features(m, _):
        passed_on(order(2 * m)).start()
        return 0

    lax.fori_loop(1, PLANE, pass_features, 0)

    scale = 1.0 / math.sqrt(width)
    tile = 128

    loads[3].wait()

    def pair_step(m, _):
        near = order(2 * m)
        far = near + Z_BIT

        @pl.when(m > 0)
        def _():
            payload_copy(near).wait_recv()
            feature_copy(features_ref, near).wait_recv()
            passed_on(near).wait_recv()

        payload_copy(far).wait_recv()
        vectors = jnp.concatenate([feats[near], feats[far]], axis=0)
        both = (near, far)

        for slot in range(own_slots):
            rows = slice(slot * HOTS, (slot + 1) * HOTS)
            low, chunk, total = [], [], []
            for source in both:
                code = recv[source, rows, :].astype(jnp.int32)
                high = jnp.zeros_like(code)
                for level in range(8, 8 + (vocab - 1) // 128):
                    high = high + (code >= (1 << level)).astype(jnp.int32)
                rest = jnp.right_shift(code, high) - 128
                low.append(rest & 7)
                chunk.append(high * 16 + jnp.right_shift(rest, 3))
                total.append(jnp.zeros((HOTS, LANES), jnp.float32))
            for part in range(vocab // tile):
                dots = lax.dot_general(
                    tables_ref[slot, part * tile : (part + 1) * tile, :], vectors,
                    (((1,), (1,)), ((), ())), preferred_element_type=jnp.float32,
                )
                for row in range(tile // HOTS):
                    at = part * (tile // HOTS) + row
                    for side in range(2):
                        found = gather_rows(
                            dots[row * HOTS : (row + 1) * HOTS, side * LANES : (side + 1) * LANES],
                            low[side],
                        )
                        total[side] = jnp.where(chunk[side] == at, found, total[side])
            weight_rows = slice(lines + slot * HOTS, lines + (slot + 1) * HOTS)
            for side, source in enumerate(both):
                weighed = total[side] * recv[source, weight_rows, :].astype(jnp.float32)
                summed[side, slot : slot + 1, :] = jnp.sum(weighed, axis=0, keepdims=True) * scale

        back[near] = summed[0].astype(jnp.bfloat16)
        back[far] = summed[1].astype(jnp.bfloat16)

        @pl.when(m > 0)
        def _():
            score_copy(near).start()

        score_copy(far).start()
        return 0

    lax.fori_loop(0, PLANE, pair_step, 0)
    scores_ref[tab] = back[0]

    def finish(offset, _):
        payload_copy(offset).wait_send()
        score_copy(offset).wait_send()
        score_copy(offset).wait_recv()
        return 0

    lax.fori_loop(1, peers, finish, 0)
    feature_copy(features_ref, Z_BIT).wait_send()

    def finish_features(m, _):
        feature_copy(features_ref, order(2 * m)).wait_send()
        passed_on(order(2 * m)).wait_send()
        return 0

    lax.fori_loop(1, PLANE, finish_features, 0)


def plane_peer(grp, tab, k):
    return {"grp": grp, "tab": flip(tab, (k // 4) * 8 + k % 4, 5)}


def column_peer(grp, tab, k):
    return {"grp": flip(grp, (k % 4) * 2, 3), "tab": flip(tab, (k // 4) * Z_BIT, 5)}


def top_kernel(
    samples_all,
    slots_ref, scores_ref, labels_ref, top_ref, bias_ref, out_ref,
    logits_ref, grad_ref, grad_bias_ref,
    grad, half_send, half_recv, plane_send, plane_recv, piece, line_send, line_recv, line_all, block, plane_all, half_all,
    bias_part, bias_half, bias_sum, bias_plane, bias_sum_two, bias_line,
    half_sem, plane_ssem, plane_rsem, line_ssem, line_rsem, lall_ssem, lall_rsem, pall_ssem, pall_rsem, hall_ssem, hall_rsem,
    bhalf_sem, bplane_ssem, bplane_rsem, bline_ssem, bline_rsem,
):
    grp, tab = place()
    core = grp % 2
    xy = (tab // 8) * 4 + tab % 4
    z = ((tab // Z_BIT) % 2) * 4 + grp // 2
    partner = {"grp": flip(grp, 1, 3), "tab": tab}
    barrier = pltpu.get_barrier_semaphore()
    pl.semaphore_signal(barrier, inc=1, device_id=partner, device_id_type=MESH)

    def greet_plane(k, _):
        pl.semaphore_signal(barrier, inc=1, device_id=plane_peer(grp, tab, k), device_id_type=MESH)
        return 0

    def greet_column(k, _):
        pl.semaphore_signal(barrier, inc=1, device_id=column_peer(grp, tab, k), device_id_type=MESH)
        return 0

    lax.fori_loop(1, 16, greet_plane, 0)
    lax.fori_loop(1, 8, greet_column, 0)

    tables, hidden_size = top_ref.shape
    at_table = (lax.broadcasted_iota(jnp.int32, (tables, tables), 0) == slots_ref[...]).astype(jnp.bfloat16)
    scores_wide = jnp.dot(at_table, scores_ref[...], preferred_element_type=jnp.float32)
    scores_t = scores_wide.astype(jnp.bfloat16)
    scores = scores_wide.T.astype(jnp.bfloat16)
    pre = jnp.dot(scores, top_ref[...], preferred_element_type=jnp.float32) + bias_ref[...]
    gate = jax.nn.sigmoid(pre)
    hidden = (pre * gate).astype(jnp.bfloat16)
    out_row = out_ref[...]
    out_wide = out_row.astype(jnp.float32)
    logit_column = jnp.sum(hidden.astype(jnp.float32) * out_wide, axis=1, keepdims=True)
    logits_ref[...] = logit_column
    delta = (jax.nn.sigmoid(logit_column) - labels_ref[...].astype(jnp.float32)) * (loss_scale / samples_all)
    slope = gate * (1.0 + pre * (1.0 - gate))
    hidden_grad_wide = delta * out_wide * slope
    hidden_grad = hidden_grad_wide.astype(jnp.bfloat16)
    grad[...] = jnp.dot(scores_t, hidden_grad, preferred_element_type=jnp.float32)
    bias_part[...] = jnp.sum(hidden_grad.astype(jnp.float32), axis=0, keepdims=True)

    other = pl.multiple_of((1 - core) * ROWS, ROWS)
    mine = pl.multiple_of(core * ROWS, ROWS)
    half_send[...] = grad[pl.ds(other, ROWS), :].reshape(16, 8, hidden_size).astype(jnp.bfloat16)

    pl.semaphore_wait(barrier, 1 + 15 + 7)

    def to_partner(source, target, sems):
        return pltpu.make_async_remote_copy(
            src_ref=source, dst_ref=target, send_sem=sems.at[0], recv_sem=sems.at[1],
            device_id=partner, device_id_type=MESH,
        )

    bias_swap = to_partner(bias_part, bias_half, bhalf_sem)
    half_swap = to_partner(half_send, half_recv, half_sem)
    bias_swap.start()
    half_swap.start()
    bias_swap.wait()
    bias_sum[...] = bias_part[...] + bias_half[...]
    bias_plane[pl.ds(xy, 1)] = bias_sum[...][None]

    def bias_to_plane(k):
        return pltpu.make_async_remote_copy(
            src_ref=bias_sum, dst_ref=bias_plane.at[xy],
            send_sem=bplane_ssem.at[k], recv_sem=bplane_rsem.at[k],
            device_id=plane_peer(grp, tab, k), device_id_type=MESH,
        )

    def grad_to_plane(k):
        return pltpu.make_async_remote_copy(
            src_ref=plane_send.at[k], dst_ref=plane_recv.at[k],
            send_sem=plane_ssem.at[k], recv_sem=plane_rsem.at[k],
            device_id=plane_peer(grp, tab, k), device_id_type=MESH,
        )

    half_swap.wait()

    def fold(k):
        row = pl.multiple_of(flip(xy, k, 4) * 8, 8)
        wide = half_recv[pl.ds(flip(xy, k, 4), 1)][0].astype(jnp.float32)
        return grad[pl.ds(pl.multiple_of(mine + row, 8), 8), :] + wide

    def send_plane(k, _):
        plane_send[k] = fold(k).astype(jnp.bfloat16)
        grad_to_plane(k).start()
        bias_to_plane(k).start()
        return 0

    lax.fori_loop(1, 16, send_plane, 0)
    piece[...] = fold(0)

    def add_plane(k, _):
        grad_to_plane(k).wait_recv()
        bias_to_plane(k).wait_recv()
        piece[...] += plane_recv[k].astype(jnp.float32)
        return 0

    lax.fori_loop(1, 16, add_plane, 0)

    total = bias_plane[0]
    for k in range(1, 16):
        total = total + bias_plane[k]
    bias_sum_two[...] = total
    bias_line[pl.ds(z, 1)] = total[None]

    def bias_to_line(k):
        return pltpu.make_async_remote_copy(
            src_ref=bias_sum_two, dst_ref=bias_line.at[z],
            send_sem=bline_ssem.at[k], recv_sem=bline_rsem.at[k],
            device_id=column_peer(grp, tab, k), device_id_type=MESH,
        )

    def grad_to_line(k):
        return pltpu.make_async_remote_copy(
            src_ref=line_send.at[k], dst_ref=line_recv.at[k],
            send_sem=line_ssem.at[k], recv_sem=line_rsem.at[k],
            device_id=column_peer(grp, tab, k), device_id_type=MESH,
        )

    def columns(k):
        return pl.ds(pl.multiple_of(flip(z, k, 3) * LANES, LANES), LANES)

    for k in range(1, 8):
        line_send[k] = piece[:, columns(k)]
        grad_to_line(k).start()
        bias_to_line(k).start()
    final = piece[:, columns(0)]
    for k in range(1, 8):
        grad_to_line(k).wait_recv()
        final = final + line_recv[k]
    line_all[0] = final

    def final_to_line(k):
        return pltpu.make_async_remote_copy(
            src_ref=line_all.at[0], dst_ref=line_all.at[k],
            send_sem=lall_ssem.at[k], recv_sem=lall_rsem.at[k],
            device_id=column_peer(grp, tab, k), device_id_type=MESH,
        )

    for k in range(1, 8):
        final_to_line(k).start()
    for k in range(1, 8):
        bias_to_line(k).wait_recv()
    total = bias_line[0]
    for k in range(1, 8):
        total = total + bias_line[k]
    grad_bias_ref[...] = total
    block[:, columns(0)] = final
    for k in range(1, 8):
        final_to_line(k).wait_recv()
        block[:, columns(k)] = line_all[k]
    plane_all[0] = block[...].astype(jnp.bfloat16)

    def block_to_plane(k):
        return pltpu.make_async_remote_copy(
            src_ref=plane_all.at[0], dst_ref=plane_all.at[k],
            send_sem=pall_ssem.at[k], recv_sem=pall_rsem.at[k],
            device_id=plane_peer(grp, tab, k), device_id_type=MESH,
        )

    def block_to_partner(k):
        return pltpu.make_async_remote_copy(
            src_ref=plane_all.at[k], dst_ref=half_all.at[k],
            send_sem=hall_ssem.at[k], recv_sem=hall_rsem.at[k],
            device_id=partner, device_id_type=MESH,
        )

    def start_blocks(k, _):
        block_to_plane(k).start()
        return 0

    lax.fori_loop(1, 16, start_blocks, 0)
    block_to_partner(0).start()

    def put(k, start, source):
        row = pl.multiple_of(start + flip(xy, k, 4) * 8, 8)
        grad_ref[pl.ds(row, 8), :] = source[k].astype(jnp.float32)

    put(0, mine, plane_all)

    def take_blocks(k, _):
        block_to_plane(k).wait_recv()
        block_to_partner(k).start()
        put(k, mine, plane_all)
        return 0

    lax.fori_loop(1, 16, take_blocks, 0)

    def take_halves(k, _):
        block_to_partner(k).wait_recv()
        put(k, other, half_all)
        block_to_partner(k).wait_send()
        return 0

    lax.fori_loop(0, 16, take_halves, 0)

    def finish_plane(k, _):
        grad_to_plane(k).wait_send()
        bias_to_plane(k).wait_send()
        block_to_plane(k).wait_send()
        return 0

    lax.fori_loop(1, 16, finish_plane, 0)
    for k in range(1, 8):
        grad_to_line(k).wait_send()
        bias_to_line(k).wait_send()
        final_to_line(k).wait_send()


def per_device(
    sample_ids, id_weights, dense_features, click_labels, table_shards, slot_table, top_weight, top_bias, out_weight,
):
    micro, local, columns = sample_ids.shape
    count = micro * local
    width = dense_features.shape[2]
    own_slots, vocab, _ = table_shards.shape
    tables, hidden_size = top_weight.shape
    peers = tables // own_slots
    samples_all = count * lax.axis_size("grp") * peers
    vmem, smem = pl.BlockSpec(memory_space=pltpu.VMEM), pl.BlockSpec(memory_space=pltpu.SMEM)
    anywhere = pl.BlockSpec(memory_space=pl.ANY)
    dma = pltpu.SemaphoreType.DMA
    bf16, f32 = jnp.bfloat16, jnp.float32

    scores = pl.pallas_call(
        exchange_kernel,
        out_shape=jax.ShapeDtypeStruct((peers, own_slots, count), bf16),
        in_specs=[smem, anywhere, anywhere, anywhere, anywhere],
        out_specs=vmem,
        scratch_shapes=[
            pltpu.VMEM((count, columns), jnp.int32),
            pltpu.VMEM((count, columns), bf16),
            pltpu.VMEM((count, width), bf16),
            pltpu.VMEM((own_slots, vocab, width), bf16),
            pltpu.VMEM((tables, HOTS, count), f32),
            pltpu.VMEM((tables, HOTS, count), f32),
            pltpu.VMEM((peers, 2 * own_slots * HOTS, count), bf16),
            pltpu.VMEM((peers, 2 * own_slots * HOTS, count), bf16),
            pltpu.VMEM((peers, count, width), bf16),
            pltpu.VMEM((peers, own_slots, count), bf16),
            pltpu.VMEM((2, own_slots, count), f32),
            dma((4,)),
        ] + [dma((peers,)) for _ in range(6)],
        compiler_params=pltpu.CompilerParams(collective_id=0, has_side_effects=True, vmem_limit_bytes=60 << 20),
        name="exchange",
    )(
        slot_table,
        sample_ids.reshape(count, columns),
        id_weights.reshape(count, columns),
        dense_features.reshape(count, width),
        table_shards,
    )

    logits, grad_top, grad_bias = pl.pallas_call(
        functools.partial(top_kernel, samples_all),
        out_shape=(
            jax.ShapeDtypeStruct((count, 1), f32),
            jax.ShapeDtypeStruct((tables, hidden_size), f32),
            jax.ShapeDtypeStruct((1, hidden_size), f32),
        ),
        in_specs=[vmem] * 6,
        out_specs=(vmem, vmem, vmem),
        scratch_shapes=[
            pltpu.VMEM((tables, hidden_size), f32),
            pltpu.VMEM((16, 8, hidden_size), bf16),
            pltpu.VMEM((16, 8, hidden_size), bf16),
            pltpu.VMEM((16, 8, hidden_size), bf16),
            pltpu.VMEM((16, 8, hidden_size), bf16),
            pltpu.VMEM((8, hidden_size), f32),
            pltpu.VMEM((8, 8, LANES), f32),
            pltpu.VMEM((8, 8, LANES), f32),
            pltpu.VMEM((8, 8, LANES), f32),
            pltpu.VMEM((8, hidden_size), f32),
            pltpu.VMEM((16, 8, hidden_size), bf16),
            pltpu.VMEM((16, 8, hidden_size), bf16),
            pltpu.VMEM((1, hidden_size), f32),
            pltpu.VMEM((1, hidden_size), f32),
            pltpu.VMEM((1, hidden_size), f32),
            pltpu.VMEM((16, 1, hidden_size), f32),
            pltpu.VMEM((1, hidden_size), f32),
            pltpu.VMEM((8, 1, hidden_size), f32),
            dma((2,)), dma((16,)), dma((16,)), dma((8,)), dma((8,)), dma((8,)), dma((8,)),
            dma((16,)), dma((16,)), dma((16,)), dma((16,)),
            dma((2,)), dma((16,)), dma((16,)), dma((8,)), dma((8,)),
        ],
        compiler_params=pltpu.CompilerParams(collective_id=1, has_side_effects=True, vmem_limit_bytes=48 << 20),
        name="top",
    )(
        slot_table.reshape(1, tables),
        scores.reshape(tables, count),
        click_labels.reshape(count, 1),
        top_weight,
        top_bias.reshape(1, hidden_size),
        out_weight.reshape(1, hidden_size),
    )
    return logits.reshape(micro, local), grad_top, grad_bias.reshape(hidden_size)


def solution(mesh):
    return jax.shard_map(
        per_device,
        mesh=mesh,
        in_specs=(
            P(None, ("grp", "tab"), None),
            P(None, ("grp", "tab"), None),
            P(None, ("grp", "tab"), None),
            P(None, ("grp", "tab")),
            P("tab", None, None),
            P(),
            P(),
            P(),
            P(),
        ),
        out_specs=(P(None, ("grp", "tab")), P(), P()),
        check_vma=False,
    )
```

```python
import functools
import math

import jax
import jax.numpy as jnp
from jax import lax
from jax.experimental import pallas as pl
from jax.experimental.pallas import tpu as pltpu
from jax.sharding import PartitionSpec as P

HOTS = 8
LANES = 128
MESH = pl.DeviceIdType.MESH
loss_scale = 32768.0

Z_BIT = 4
PLANE = 16
ROWS = 128


def place():
    grp, tab = lax.axis_index("grp"), lax.axis_index("tab")
    return grp, tab


def mirrored(grp):
    return (3 - grp // 2) * 2 + grp % 2


def order(step):
    return (step // 8) * 8 + (step % 2) * Z_BIT + (step // 2) % 4


def plane(at):
    return (at // 4) * 8 + at % 4


def flip(value, offset, bits):
    total = 0
    for bit in range(bits):
        unit = 1 << bit
        one, two = (value // unit) % 2, (offset // unit) % 2
        total = total + (one + two - 2 * one * two) * unit
    return total


def peer_of(grp, tab, offset):
    cross = (offset // Z_BIT) % 2
    there = cross * mirrored(grp) + (1 - cross) * grp
    return {"grp": there, "tab": flip(tab, offset, 5)}


def gather_rows(source, index):
    dims = lax.GatherDimensionNumbers(
        offset_dims=(),
        collapsed_slice_dims=(0,),
        start_index_map=(0,),
        operand_batching_dims=(1,),
        start_indices_batching_dims=(1,),
    )
    return lax.gather(
        source, index[..., None], dims, slice_sizes=(1, 1),
        mode=lax.GatherScatterMode.PROMISE_IN_BOUNDS,
    )


def plane_peer(grp, tab, k):
    return {"grp": grp, "tab": flip(tab, (k // 4) * 8 + k % 4, 5)}


def column_peer(grp, tab, k):
    return {"grp": flip(grp, (k % 4) * 2, 3), "tab": flip(tab, (k // 4) * Z_BIT, 5)}


def step_kernel(
    samples_all,
    slots_ref, slots_hbm, ids_hbm, weights_hbm, features_hbm, tables_hbm, labels_hbm, top_hbm, bias_hbm, out_hbm,
    logits_ref, grad_ref, grad_bias_ref,
    ids_ref, weights_ref, features_ref, tables_ref, slot_row, labels_ref, top_ref, bias_ref, out_ref,
    ids_t, weights_t, send, recv, feats, back, summed, scores_ref,
    grad, half_send, half_recv, plane_send, plane_recv, piece, line_send, line_recv, plane_all, half_all,
    bias_part, bias_half, bias_sum, bias_plane, bias_sum_two, bias_line,
    load_sem, send_sem, recv_sem, fsend_sem, frecv_sem, bsend_sem, brecv_sem,
    half_sem, plane_ssem, plane_rsem, line_ssem, line_rsem, pall_ssem, pall_rsem, hall_ssem, hall_rsem,
    bhalf_sem, bplane_ssem, bplane_rsem, bline_ssem, bline_rsem,
):
    grp, tab = place()
    peers = send.shape[0]
    own_slots, vocab, width = tables_ref.shape
    lines = own_slots * HOTS
    loads = [
        pltpu.make_async_copy(source, target, load_sem.at[at])
        for at, (source, target) in enumerate(
            [
                (features_hbm, features_ref), (ids_hbm, ids_ref), (weights_hbm, weights_ref), (tables_hbm, tables_ref),
                (slots_hbm, slot_row), (labels_hbm, labels_ref), (top_hbm, top_ref), (bias_hbm, bias_ref), (out_hbm, out_ref),
            ]
        )
    ]
    for load in loads:
        load.start()
    barrier = pltpu.get_barrier_semaphore()

    def greet(offset, _):
        pl.semaphore_signal(barrier, inc=1, device_id=peer_of(grp, tab, offset), device_id_type=MESH)
        return 0

    def greet_column(k, _):
        pl.semaphore_signal(barrier, inc=1, device_id=column_peer(grp, tab, k), device_id_type=MESH)
        return 0

    partner = {"grp": flip(grp, 1, 3), "tab": tab}
    lax.fori_loop(1, peers, greet, 0)
    lax.fori_loop(1, 8, greet_column, 0)
    pl.semaphore_signal(barrier, inc=1, device_id=partner, device_id_type=MESH)
    loads[0].wait()
    feats[0] = features_ref[...]
    loads[1].wait()
    loads[2].wait()
    per_block = LANES // HOTS
    for at in range(ids_ref.shape[1] // LANES):
        columns = slice(at * LANES, (at + 1) * LANES)
        held = slice(at * per_block, (at + 1) * per_block)
        ids = ids_ref[:, columns]
        code = jnp.left_shift((ids & 127) + 128, jnp.right_shift(ids, 7))
        ids_t[held] = code.astype(jnp.float32).T.reshape(per_block, HOTS, LANES)
        weights_t[held] = weights_ref[:, columns].astype(jnp.float32).T.reshape(per_block, HOTS, LANES)

    def packed(offset, target):
        first = flip(tab, offset, 5) * own_slots
        for pair in range(own_slots // 2):
            one, two = slots_ref[first + 2 * pair], slots_ref[first + 2 * pair + 1]
            rows = slice(pair * 2 * HOTS, (pair + 1) * 2 * HOTS)
            target[offset, rows, :] = jnp.concatenate([ids_t[one], ids_t[two]], axis=0).astype(jnp.bfloat16)
            rows = slice(lines + pair * 2 * HOTS, lines + (pair + 1) * 2 * HOTS)
            target[offset, rows, :] = jnp.concatenate([weights_t[one], weights_t[two]], axis=0).astype(jnp.bfloat16)

    packed(0, recv)
    pl.semaphore_wait(barrier, peers - 1 + 7 + 1)

    def feature_copy(source, offset):
        return pltpu.make_async_remote_copy(
            src_ref=source, dst_ref=feats.at[offset],
            send_sem=fsend_sem.at[offset], recv_sem=frecv_sem.at[offset],
            device_id=peer_of(grp, tab, offset), device_id_type=MESH,
        )

    def passed_on(offset):
        return pltpu.make_async_remote_copy(
            src_ref=feats.at[Z_BIT], dst_ref=feats.at[offset + Z_BIT],
            send_sem=fsend_sem.at[offset + Z_BIT], recv_sem=frecv_sem.at[offset + Z_BIT],
            device_id=peer_of(grp, tab, offset), device_id_type=MESH,
        )

    def payload_copy(offset):
        return pltpu.make_async_remote_copy(
            src_ref=send.at[offset], dst_ref=recv.at[offset],
            send_sem=send_sem.at[offset], recv_sem=recv_sem.at[offset],
            device_id=peer_of(grp, tab, offset), device_id_type=MESH,
        )

    def score_copy(offset):
        return pltpu.make_async_remote_copy(
            src_ref=back.at[offset], dst_ref=scores_ref.at[tab],
            send_sem=bsend_sem.at[offset], recv_sem=brecv_sem.at[offset],
            device_id=peer_of(grp, tab, offset), device_id_type=MESH,
        )

    feature_copy(features_ref, Z_BIT).start()

    def send_features(m, _):
        feature_copy(features_ref, order(2 * m)).start()
        return 0

    lax.fori_loop(1, PLANE, send_features, 0)


    def send_payload(step, _):
        offset = order(step)
        packed(offset, send)
        payload_copy(offset).start()
        return 0

    lax.fori_loop(1, peers, send_payload, 0)
    def pass_features(m, _):
        passed_on(order(2 * m)).start()
        return 0

    scale = 1.0 / math.sqrt(width)
    tile = 128

    loads[3].wait()

    def pair_step(m, _):
        both = [plane(2 * (m % 8) + side) + (m // 8) * Z_BIT for side in range(2)]

        @pl.when(m > 0)
        def _():
            payload_copy(both[0]).wait_recv()

        @pl.when(m % 8 > 0)
        def _():
            feature_copy(features_ref, both[0]).wait_recv()

        payload_copy(both[1]).wait_recv()
        feature_copy(features_ref, both[1]).wait_recv()
        vectors = jnp.concatenate([feats[both[0]], feats[both[1]]], axis=0)

        for slot in range(own_slots):
            rows = slice(slot * HOTS, (slot + 1) * HOTS)
            low, chunk, total = [], [], []
            for source in both:
                code = recv[source, rows, :].astype(jnp.int32)
                high = jnp.zeros_like(code)
                for level in range(8, 8 + (vocab - 1) // 128):
                    high = high + (code >= (1 << level)).astype(jnp.int32)
                rest = jnp.right_shift(code, high) - 128
                low.append(rest & 7)
                chunk.append(high * 16 + jnp.right_shift(rest, 3))
                total.append(jnp.zeros((HOTS, LANES), jnp.float32))
            for part in range(vocab // tile):
                dots = lax.dot_general(
                    tables_ref[slot, part * tile : (part + 1) * tile, :], vectors,
                    (((1,), (1,)), ((), ())), preferred_element_type=jnp.float32,
                )
                for row in range(tile // HOTS):
                    at = part * (tile // HOTS) + row
                    for side in range(2):
                        found = gather_rows(
                            dots[row * HOTS : (row + 1) * HOTS, side * LANES : (side + 1) * LANES],
                            low[side],
                        )
                        total[side] = jnp.where(chunk[side] == at, found, total[side])
            weight_rows = slice(lines + slot * HOTS, lines + (slot + 1) * HOTS)
            for side, source in enumerate(both):
                weighed = total[side] * recv[source, weight_rows, :].astype(jnp.float32)
                summed[side, slot : slot + 1, :] = jnp.sum(weighed, axis=0, keepdims=True) * scale

        for side in range(2):
            back[both[side]] = summed[side].astype(jnp.bfloat16)

        @pl.when(m > 0)
        def _():
            score_copy(both[0]).start()

        score_copy(both[1]).start()

        @pl.when(m == 0)
        def _():
            feature_copy(features_ref, Z_BIT).wait_recv()
            lax.fori_loop(1, PLANE, pass_features, 0)

        return 0

    lax.fori_loop(0, PLANE, pair_step, 0)
    scores_ref[tab] = back[0]

    for load in loads[4:]:
        load.wait()

    def take_scores(offset, _):
        score_copy(offset).wait_recv()
        return 0

    lax.fori_loop(1, peers, take_scores, 0)

    core = grp % 2
    xy = (tab // 8) * 4 + tab % 4
    z = ((tab // Z_BIT) % 2) * 4 + grp // 2
    tables, hidden_size = top_ref.shape
    at_table = (lax.broadcasted_iota(jnp.int32, (tables, tables), 0) == slot_row[...]).astype(jnp.bfloat16)
    scores_wide = jnp.dot(at_table, scores_ref[...].reshape(tables, LANES), preferred_element_type=jnp.float32)
    scores_t = scores_wide.astype(jnp.bfloat16)
    scores = scores_wide.T.astype(jnp.bfloat16)
    pre = jnp.dot(scores, top_ref[...], preferred_element_type=jnp.float32) + bias_ref[...]
    gate = jax.nn.sigmoid(pre)
    hidden = (pre * gate).astype(jnp.bfloat16)
    out_wide = out_ref[...].astype(jnp.float32).reshape(1, hidden_size)
    logit_column = jnp.sum(hidden.astype(jnp.float32) * out_wide, axis=1, keepdims=True)
    micro, local = labels_ref.shape
    sample = lax.broadcasted_iota(jnp.int32, (LANES, local), 0)
    within = sample % local == lax.broadcasted_iota(jnp.int32, (LANES, local), 1)
    batch_of = lax.broadcasted_iota(jnp.int32, (LANES, micro), 0) // local
    spread = lax.dot_general(
        within.astype(jnp.float32), labels_ref[...].astype(jnp.float32),
        (((1,), (1,)), ((), ())), preferred_element_type=jnp.float32,
    )
    own_batch = batch_of == lax.broadcasted_iota(jnp.int32, (LANES, micro), 1)
    labels = jnp.sum(jnp.where(own_batch, spread, 0.0), axis=1, keepdims=True)
    rows_of = lax.broadcasted_iota(jnp.int32, (micro, LANES), 1) // local
    picks = (rows_of == lax.broadcasted_iota(jnp.int32, (micro, LANES), 0)).astype(jnp.float32)
    logits_ref[...] = jnp.dot(
        picks, jnp.where(within, logit_column, 0.0),
        precision=lax.Precision.HIGHEST, preferred_element_type=jnp.float32,
    )
    delta = (jax.nn.sigmoid(logit_column) - labels) * (loss_scale / samples_all)
    slope = gate * (1.0 + pre * (1.0 - gate))
    hidden_grad_wide = delta * out_wide * slope
    hidden_grad = hidden_grad_wide.astype(jnp.bfloat16)
    grad[...] = jnp.dot(scores_t, hidden_grad, preferred_element_type=jnp.float32)
    bias_part[...] = jnp.sum(hidden_grad.astype(jnp.float32), axis=0, keepdims=True)

    other = pl.multiple_of((1 - core) * ROWS, ROWS)
    mine = pl.multiple_of(core * ROWS, ROWS)
    half_send[...] = grad[pl.ds(other, ROWS), :].reshape(16, 8, hidden_size).astype(jnp.bfloat16)

    def to_partner(source, target, sems):
        return pltpu.make_async_remote_copy(
            src_ref=source, dst_ref=target, send_sem=sems.at[0], recv_sem=sems.at[1],
            device_id=partner, device_id_type=MESH,
        )

    bias_swap = to_partner(bias_part, bias_half, bhalf_sem)
    half_swap = to_partner(half_send, half_recv, half_sem)
    bias_swap.start()
    half_swap.start()
    bias_swap.wait()
    bias_sum[...] = bias_part[...] + bias_half[...]
    bias_plane[pl.ds(xy, 1)] = bias_sum[...][None]

    def bias_to_plane(k):
        return pltpu.make_async_remote_copy(
            src_ref=bias_sum, dst_ref=bias_plane.at[xy],
            send_sem=bplane_ssem.at[k], recv_sem=bplane_rsem.at[k],
            device_id=plane_peer(grp, tab, k), device_id_type=MESH,
        )

    def grad_to_plane(k):
        return pltpu.make_async_remote_copy(
            src_ref=plane_send.at[k], dst_ref=plane_recv.at[k],
            send_sem=plane_ssem.at[k], recv_sem=plane_rsem.at[k],
            device_id=plane_peer(grp, tab, k), device_id_type=MESH,
        )

    half_swap.wait()

    def fold(k):
        row = pl.multiple_of(flip(xy, k, 4) * 8, 8)
        wide = half_recv[pl.ds(flip(xy, k, 4), 1)][0].astype(jnp.float32)
        return grad[pl.ds(pl.multiple_of(mine + row, 8), 8), :] + wide

    def send_plane(k, _):
        plane_send[k] = fold(k).astype(jnp.bfloat16)
        grad_to_plane(k).start()
        bias_to_plane(k).start()
        return 0

    lax.fori_loop(1, 16, send_plane, 0)
    piece[...] = fold(0)

    def add_plane(k, _):
        grad_to_plane(k).wait_recv()
        bias_to_plane(k).wait_recv()
        piece[...] += plane_recv[k].astype(jnp.float32)
        return 0

    lax.fori_loop(1, 16, add_plane, 0)

    def grad_to_line(k):
        return pltpu.make_async_remote_copy(
            src_ref=line_send, dst_ref=line_recv.at[z],
            send_sem=line_ssem.at[k], recv_sem=line_rsem.at[k],
            device_id=column_peer(grp, tab, k), device_id_type=MESH,
        )

    line_send[...] = piece[...].astype(jnp.bfloat16)
    line_recv[pl.ds(z, 1)] = piece[...].astype(jnp.bfloat16)[None]
    for k in range(1, 8):
        grad_to_line(k).start()
    total = bias_plane[0]
    for k in range(1, 16):
        total = total + bias_plane[k]
    bias_sum_two[...] = total
    bias_line[pl.ds(z, 1)] = total[None]

    def bias_to_line(k):
        return pltpu.make_async_remote_copy(
            src_ref=bias_sum_two, dst_ref=bias_line.at[z],
            send_sem=bline_ssem.at[k], recv_sem=bline_rsem.at[k],
            device_id=column_peer(grp, tab, k), device_id_type=MESH,
        )

    for k in range(1, 8):
        bias_to_line(k).start()
    for k in range(1, 8):
        grad_to_line(k).wait_recv()
    block = line_recv[0].astype(jnp.float32)
    for k in range(1, 8):
        block = block + line_recv[k].astype(jnp.float32)
    plane_all[0] = block.astype(jnp.bfloat16)

    def block_to_plane(k):
        return pltpu.make_async_remote_copy(
            src_ref=plane_all.at[0], dst_ref=plane_all.at[k],
            send_sem=pall_ssem.at[k], recv_sem=pall_rsem.at[k],
            device_id=plane_peer(grp, tab, k), device_id_type=MESH,
        )

    def block_to_partner(k):
        return pltpu.make_async_remote_copy(
            src_ref=plane_all.at[k], dst_ref=half_all.at[k],
            send_sem=hall_ssem.at[k], recv_sem=hall_rsem.at[k],
            device_id=partner, device_id_type=MESH,
        )

    def start_blocks(k, _):
        block_to_plane(k).start()
        return 0

    lax.fori_loop(1, 16, start_blocks, 0)
    block_to_partner(0).start()
    for k in range(1, 8):
        bias_to_line(k).wait_recv()
    total = bias_line[0]
    for k in range(1, 8):
        total = total + bias_line[k]
    grad_bias_ref[...] = total

    def put(k, start, source):
        row = pl.multiple_of(start + flip(xy, k, 4) * 8, 8)
        grad_ref[pl.ds(row, 8), :] = source[k].astype(jnp.float32)

    put(0, mine, plane_all)

    def take_blocks(k, _):
        block_to_plane(k).wait_recv()
        block_to_partner(k).start()
        put(k, mine, plane_all)
        return 0

    lax.fori_loop(1, 16, take_blocks, 0)

    def take_halves(k, _):
        block_to_partner(k).wait_recv()
        put(k, other, half_all)
        block_to_partner(k).wait_send()
        return 0

    lax.fori_loop(0, 16, take_halves, 0)

    def finish_plane(k, _):
        grad_to_plane(k).wait_send()
        bias_to_plane(k).wait_send()
        block_to_plane(k).wait_send()
        return 0

    lax.fori_loop(1, 16, finish_plane, 0)
    for k in range(1, 8):
        grad_to_line(k).wait_send()
        bias_to_line(k).wait_send()

    def finish(offset, _):
        payload_copy(offset).wait_send()
        score_copy(offset).wait_send()
        return 0

    lax.fori_loop(1, peers, finish, 0)
    feature_copy(features_ref, Z_BIT).wait_send()

    def finish_features(m, _):
        feature_copy(features_ref, order(2 * m)).wait_send()
        passed_on(order(2 * m)).wait_send()
        return 0

    lax.fori_loop(1, PLANE, finish_features, 0)


def per_device(
    sample_ids, id_weights, dense_features, click_labels, table_shards, slot_table, top_weight, top_bias, out_weight,
):
    micro, local, columns = sample_ids.shape
    count = micro * local
    width = dense_features.shape[2]
    own_slots, vocab, _ = table_shards.shape
    tables, hidden_size = top_weight.shape
    peers = tables // own_slots
    samples_all = count * lax.axis_size("grp") * peers
    vmem, smem = pl.BlockSpec(memory_space=pltpu.VMEM), pl.BlockSpec(memory_space=pltpu.SMEM)
    anywhere = pl.BlockSpec(memory_space=pl.ANY)
    dma = pltpu.SemaphoreType.DMA
    bf16, f32 = jnp.bfloat16, jnp.float32

    logits, grad_top, grad_bias = pl.pallas_call(
        functools.partial(step_kernel, samples_all),
        out_shape=(
            jax.ShapeDtypeStruct((micro, local), f32),
            jax.ShapeDtypeStruct((tables, hidden_size), f32),
            jax.ShapeDtypeStruct((1, hidden_size), f32),
        ),
        in_specs=[smem] + [anywhere] * 9,
        out_specs=(vmem, vmem, vmem),
        scratch_shapes=[
            pltpu.VMEM((count, columns), jnp.int32),
            pltpu.VMEM((count, columns), bf16),
            pltpu.VMEM((count, width), bf16),
            pltpu.VMEM((own_slots, vocab, width), bf16),
            pltpu.VMEM((1, tables), jnp.int32),
            pltpu.VMEM((micro, local), jnp.int32),
            pltpu.VMEM((tables, hidden_size), bf16),
            pltpu.VMEM((1, hidden_size), f32),
            pltpu.VMEM((hidden_size,), bf16),
            pltpu.VMEM((tables, HOTS, count), f32),
            pltpu.VMEM((tables, HOTS, count), f32),
            pltpu.VMEM((peers, 2 * own_slots * HOTS, count), bf16),
            pltpu.VMEM((peers, 2 * own_slots * HOTS, count), bf16),
            pltpu.VMEM((peers, count, width), bf16),
            pltpu.VMEM((peers, own_slots, count), bf16),
            pltpu.VMEM((2, own_slots, count), f32),
            pltpu.VMEM((peers, own_slots, count), bf16),
            pltpu.VMEM((tables, hidden_size), f32),
            pltpu.VMEM((16, 8, hidden_size), bf16),
            pltpu.VMEM((16, 8, hidden_size), bf16),
            pltpu.VMEM((16, 8, hidden_size), bf16),
            pltpu.VMEM((16, 8, hidden_size), bf16),
            pltpu.VMEM((8, hidden_size), f32),
            pltpu.VMEM((8, hidden_size), bf16),
            pltpu.VMEM((8, 8, hidden_size), bf16),
            pltpu.VMEM((16, 8, hidden_size), bf16),
            pltpu.VMEM((16, 8, hidden_size), bf16),
            pltpu.VMEM((1, hidden_size), f32),
            pltpu.VMEM((1, hidden_size), f32),
            pltpu.VMEM((1, hidden_size), f32),
            pltpu.VMEM((16, 1, hidden_size), f32),
            pltpu.VMEM((1, hidden_size), f32),
            pltpu.VMEM((8, 1, hidden_size), f32),
            dma((9,)),
        ] + [dma((peers,)) for _ in range(6)] + [
            dma((2,)), dma((16,)), dma((16,)), dma((8,)), dma((8,)),
            dma((16,)), dma((16,)), dma((16,)), dma((16,)),
            dma((2,)), dma((16,)), dma((16,)), dma((8,)), dma((8,)),
        ],
        compiler_params=pltpu.CompilerParams(collective_id=0, has_side_effects=True, vmem_limit_bytes=60 << 20),
        name="step",
    )(
        slot_table,
        slot_table.reshape(1, tables),
        sample_ids.reshape(count, columns),
        id_weights.reshape(count, columns),
        dense_features.reshape(count, width),
        table_shards,
        click_labels,
        top_weight,
        top_bias.reshape(1, hidden_size),
        out_weight,
    )
    return logits, grad_top, grad_bias.reshape(hidden_size)


def solution(mesh):
    return jax.shard_map(
        per_device,
        mesh=mesh,
        in_specs=(
            P(None, ("grp", "tab"), None),
            P(None, ("grp", "tab"), None),
            P(None, ("grp", "tab"), None),
            P(None, ("grp", "tab")),
            P("tab", None, None),
            P(),
            P(),
            P(),
            P(),
        ),
        out_specs=(P(None, ("grp", "tab")), P(), P()),
        check_vma=False,
    )
```

```python
import functools
import math

import jax
import jax.numpy as jnp
from jax import lax
from jax.experimental import pallas as pl
from jax.experimental.pallas import tpu as pltpu
from jax.sharding import PartitionSpec as P

HOTS = 8
LANES = 128
MESH = pl.DeviceIdType.MESH
loss_scale = 32768.0

Z_BIT = 4
PLANE = 16
ROWS = 128
FIRST_NEAR = 8
FIRST_FAR = 4
FAR_RATE = 1
PASS_AT = 4


def place():
    grp, tab = lax.axis_index("grp"), lax.axis_index("tab")
    return grp, tab


def mirrored(grp):
    return (3 - grp // 2) * 2 + grp % 2


def plane(at):
    return (at // 4) * 8 + at % 4


def flip(value, offset, bits):
    total = 0
    for bit in range(bits):
        unit = 1 << bit
        one, two = (value // unit) % 2, (offset // unit) % 2
        total = total + (one + two - 2 * one * two) * unit
    return total


def peer_of(grp, tab, offset):
    cross = (offset // Z_BIT) % 2
    there = cross * mirrored(grp) + (1 - cross) * grp
    return {"grp": there, "tab": flip(tab, offset, 5)}


def gather_rows(source, index):
    dims = lax.GatherDimensionNumbers(
        offset_dims=(),
        collapsed_slice_dims=(0,),
        start_index_map=(0,),
        operand_batching_dims=(1,),
        start_indices_batching_dims=(1,),
    )
    return lax.gather(
        source, index[..., None], dims, slice_sizes=(1, 1),
        mode=lax.GatherScatterMode.PROMISE_IN_BOUNDS,
    )


def plane_peer(grp, tab, k):
    return {"grp": grp, "tab": flip(tab, (k // 4) * 8 + k % 4, 5)}


def column_peer(grp, tab, k):
    return {"grp": flip(grp, (k % 4) * 2, 3), "tab": flip(tab, (k // 4) * Z_BIT, 5)}


def step_kernel(
    samples_all,
    slots_ref, slots_hbm, ids_hbm, weights_hbm, features_hbm, tables_hbm, labels_hbm, top_hbm, bias_hbm, out_hbm,
    logits_ref, grad_ref, grad_bias_ref,
    ids_ref, weights_ref, features_ref, tables_ref, slot_row, labels_ref, top_ref, bias_ref, out_ref,
    ids_t, weights_t, send, recv, feats, back, summed, scores_ref,
    grad, half_send, half_recv, plane_send, plane_recv, piece, line_send, line_recv, plane_all, half_all,
    bias_part, bias_half, bias_sum, bias_plane, bias_sum_two, bias_line,
    load_sem, send_sem, recv_sem, fsend_sem, frecv_sem, bsend_sem, brecv_sem,
    half_sem, plane_ssem, plane_rsem, line_ssem, line_rsem, pall_ssem, pall_rsem, hall_ssem, hall_rsem,
    bhalf_sem, bplane_ssem, bplane_rsem, bline_ssem, bline_rsem,
):
    grp, tab = place()
    peers = send.shape[0]
    own_slots, vocab, width = tables_ref.shape
    lines = own_slots * HOTS
    loads = [
        pltpu.make_async_copy(source, target, load_sem.at[at])
        for at, (source, target) in enumerate(
            [
                (features_hbm, features_ref), (ids_hbm, ids_ref), (weights_hbm, weights_ref), (tables_hbm, tables_ref),
                (slots_hbm, slot_row), (labels_hbm, labels_ref), (top_hbm, top_ref), (bias_hbm, bias_ref), (out_hbm, out_ref),
            ]
        )
    ]
    for load in loads:
        load.start()
    barrier = pltpu.get_barrier_semaphore()

    def greet(offset, _):
        pl.semaphore_signal(barrier, inc=1, device_id=peer_of(grp, tab, offset), device_id_type=MESH)
        return 0

    def greet_column(k, _):
        pl.semaphore_signal(barrier, inc=1, device_id=column_peer(grp, tab, k), device_id_type=MESH)
        return 0

    partner = {"grp": flip(grp, 1, 3), "tab": tab}
    lax.fori_loop(1, peers, greet, 0)
    lax.fori_loop(1, 8, greet_column, 0)
    pl.semaphore_signal(barrier, inc=1, device_id=partner, device_id_type=MESH)
    loads[0].wait()
    feats[0] = features_ref[...]
    loads[1].wait()
    loads[2].wait()
    per_block = LANES // HOTS
    for at in range(ids_ref.shape[1] // LANES):
        columns = slice(at * LANES, (at + 1) * LANES)
        held = slice(at * per_block, (at + 1) * per_block)
        ids = ids_ref[:, columns]
        code = jnp.left_shift((ids & 127) + 128, jnp.right_shift(ids, 7))
        ids_t[held] = code.astype(jnp.float32).T.reshape(per_block, HOTS, LANES)
        weights_t[held] = weights_ref[:, columns].astype(jnp.float32).T.reshape(per_block, HOTS, LANES)

    def packed(offset, target):
        first = flip(tab, offset, 5) * own_slots
        for pair in range(own_slots // 2):
            one, two = slots_ref[first + 2 * pair], slots_ref[first + 2 * pair + 1]
            rows = slice(pair * 2 * HOTS, (pair + 1) * 2 * HOTS)
            target[offset, rows, :] = jnp.concatenate([ids_t[one], ids_t[two]], axis=0).astype(jnp.bfloat16)
            rows = slice(lines + pair * 2 * HOTS, lines + (pair + 1) * 2 * HOTS)
            target[offset, rows, :] = jnp.concatenate([weights_t[one], weights_t[two]], axis=0).astype(jnp.bfloat16)

    def pack_all(offset, _):
        packed(offset, send)
        return 0

    packed(0, recv)
    lax.fori_loop(1, peers, pack_all, 0)
    pl.semaphore_wait(barrier, peers - 1 + 7 + 1)

    def feature_copy(source, offset):
        return pltpu.make_async_remote_copy(
            src_ref=source, dst_ref=feats.at[offset],
            send_sem=fsend_sem.at[offset], recv_sem=frecv_sem.at[offset],
            device_id=peer_of(grp, tab, offset), device_id_type=MESH,
        )

    def passed_on(offset):
        return pltpu.make_async_remote_copy(
            src_ref=feats.at[Z_BIT], dst_ref=feats.at[offset + Z_BIT],
            send_sem=fsend_sem.at[offset + Z_BIT], recv_sem=frecv_sem.at[offset + Z_BIT],
            device_id=peer_of(grp, tab, offset), device_id_type=MESH,
        )

    def payload_copy(offset):
        return pltpu.make_async_remote_copy(
            src_ref=send.at[offset], dst_ref=recv.at[offset],
            send_sem=send_sem.at[offset], recv_sem=recv_sem.at[offset],
            device_id=peer_of(grp, tab, offset), device_id_type=MESH,
        )

    def score_copy(offset):
        return pltpu.make_async_remote_copy(
            src_ref=back.at[offset], dst_ref=scores_ref.at[tab],
            send_sem=bsend_sem.at[offset], recv_sem=brecv_sem.at[offset],
            device_id=peer_of(grp, tab, offset), device_id_type=MESH,
        )

    feature_copy(features_ref, Z_BIT).start()

    def send_near(at):
        offset = plane(at)
        feature_copy(features_ref, offset).start()
        payload_copy(offset).start()

    def send_far(at):
        offset = plane(at) + Z_BIT
        payload_copy(offset).start()

    def pass_features(at):
        passed_on(plane(at)).start()

    def first_sends(at, _):
        @pl.when(at < FIRST_NEAR)
        def _():
            send_near(at)

        @pl.when(at - 1 < FIRST_FAR)
        def _():
            send_far(at - 1)

        return 0

    lax.fori_loop(1, max(FIRST_NEAR, FIRST_FAR + 1), first_sends, 0)

    def later_sends(m):
        for side in range(2):
            near = FIRST_NEAR + 2 * m + side

            @pl.when(near < PLANE)
            def _():
                send_near(near)

        for side in range(FAR_RATE):
            far = FIRST_FAR + FAR_RATE * m + side

            @pl.when(far < PLANE)
            def _():
                send_far(far)

        @pl.when(m == PASS_AT)
        def _():
            feature_copy(features_ref, Z_BIT).wait_recv()

        for side in range(2):
            place_to = 1 + 2 * (m - PASS_AT) + side

            @pl.when((m >= PASS_AT) & (place_to < PLANE))
            def _():
                pass_features(place_to)

    scale = 1.0 / math.sqrt(width)
    tile = 128

    loads[3].wait()

    def pair_step(m, _):
        both = [plane(2 * (m % 8) + side) + (m // 8) * Z_BIT for side in range(2)]

        @pl.when(m > 0)
        def _():
            payload_copy(both[0]).wait_recv()

        @pl.when(m % 8 > 0)
        def _():
            feature_copy(features_ref, both[0]).wait_recv()

        payload_copy(both[1]).wait_recv()
        feature_copy(features_ref, both[1]).wait_recv()
        later_sends(m)
        vectors = jnp.concatenate([feats[both[0]], feats[both[1]]], axis=0)

        for slot in range(own_slots):
            rows = slice(slot * HOTS, (slot + 1) * HOTS)
            low, chunk, total = [], [], []
            for source in both:
                code = recv[source, rows, :].astype(jnp.int32)
                high = jnp.zeros_like(code)
                for level in range(8, 8 + (vocab - 1) // 128):
                    high = high + (code >= (1 << level)).astype(jnp.int32)
                rest = jnp.right_shift(code, high) - 128
                low.append(rest & 7)
                chunk.append(high * 16 + jnp.right_shift(rest, 3))
                total.append(jnp.zeros((HOTS, LANES), jnp.float32))
            for part in range(vocab // tile):
                dots = lax.dot_general(
                    tables_ref[slot, part * tile : (part + 1) * tile, :], vectors,
                    (((1,), (1,)), ((), ())), preferred_element_type=jnp.float32,
                )
                for row in range(tile // HOTS):
                    at = part * (tile // HOTS) + row
                    for side in range(2):
                        found = gather_rows(
                            dots[row * HOTS : (row + 1) * HOTS, side * LANES : (side + 1) * LANES],
                            low[side],
                        )
                        total[side] = jnp.where(chunk[side] == at, found, total[side])
            weight_rows = slice(lines + slot * HOTS, lines + (slot + 1) * HOTS)
            for side, source in enumerate(both):
                weighed = total[side] * recv[source, weight_rows, :].astype(jnp.float32)
                summed[side, slot : slot + 1, :] = jnp.sum(weighed, axis=0, keepdims=True) * scale

        for side in range(2):
            back[both[side]] = summed[side].astype(jnp.bfloat16)

        @pl.when(m > 0)
        def _():
            score_copy(both[0]).start()

        score_copy(both[1]).start()

        return 0

    lax.fori_loop(0, PLANE, pair_step, 0)
    scores_ref[tab] = back[0]

    for load in loads[4:]:
        load.wait()

    def take_scores(offset, _):
        score_copy(offset).wait_recv()
        return 0

    lax.fori_loop(1, peers, take_scores, 0)

    core = grp % 2
    xy = (tab // 8) * 4 + tab % 4
    z = ((tab // Z_BIT) % 2) * 4 + grp // 2
    tables, hidden_size = top_ref.shape
    at_table = (lax.broadcasted_iota(jnp.int32, (tables, tables), 0) == slot_row[...]).astype(jnp.bfloat16)
    scores_wide = jnp.dot(at_table, scores_ref[...].reshape(tables, LANES), preferred_element_type=jnp.float32)
    scores_t = scores_wide.astype(jnp.bfloat16)
    scores = scores_wide.T.astype(jnp.bfloat16)
    pre = jnp.dot(scores, top_ref[...], preferred_element_type=jnp.float32) + bias_ref[...]
    gate = jax.nn.sigmoid(pre)
    hidden = (pre * gate).astype(jnp.bfloat16)
    out_wide = out_ref[...].astype(jnp.float32).reshape(1, hidden_size)
    logit_column = jnp.sum(hidden.astype(jnp.float32) * out_wide, axis=1, keepdims=True)
    micro, local = labels_ref.shape
    sample = lax.broadcasted_iota(jnp.int32, (LANES, local), 0)
    within = sample % local == lax.broadcasted_iota(jnp.int32, (LANES, local), 1)
    batch_of = lax.broadcasted_iota(jnp.int32, (LANES, micro), 0) // local
    spread = lax.dot_general(
        within.astype(jnp.float32), labels_ref[...].astype(jnp.float32),
        (((1,), (1,)), ((), ())), preferred_element_type=jnp.float32,
    )
    own_batch = batch_of == lax.broadcasted_iota(jnp.int32, (LANES, micro), 1)
    labels = jnp.sum(jnp.where(own_batch, spread, 0.0), axis=1, keepdims=True)
    rows_of = lax.broadcasted_iota(jnp.int32, (micro, LANES), 1) // local
    picks = (rows_of == lax.broadcasted_iota(jnp.int32, (micro, LANES), 0)).astype(jnp.float32)
    logits_ref[...] = jnp.dot(
        picks, jnp.where(within, logit_column, 0.0),
        precision=lax.Precision.HIGHEST, preferred_element_type=jnp.float32,
    )
    delta = (jax.nn.sigmoid(logit_column) - labels) * (loss_scale / samples_all)
    slope = gate * (1.0 + pre * (1.0 - gate))
    hidden_grad_wide = delta * out_wide * slope
    hidden_grad = hidden_grad_wide.astype(jnp.bfloat16)
    grad[...] = jnp.dot(scores_t, hidden_grad, preferred_element_type=jnp.float32)
    bias_part[...] = jnp.sum(hidden_grad.astype(jnp.float32), axis=0, keepdims=True)

    other = pl.multiple_of((1 - core) * ROWS, ROWS)
    mine = pl.multiple_of(core * ROWS, ROWS)
    half_send[...] = grad[pl.ds(other, ROWS), :].reshape(16, 8, hidden_size).astype(jnp.bfloat16)

    def to_partner(source, target, sems):
        return pltpu.make_async_remote_copy(
            src_ref=source, dst_ref=target, send_sem=sems.at[0], recv_sem=sems.at[1],
            device_id=partner, device_id_type=MESH,
        )

    bias_swap = to_partner(bias_part, bias_half, bhalf_sem)
    half_swap = to_partner(half_send, half_recv, half_sem)
    bias_swap.start()
    half_swap.start()
    bias_swap.wait()
    bias_sum[...] = bias_part[...] + bias_half[...]
    bias_plane[pl.ds(xy, 1)] = bias_sum[...][None]

    def bias_to_plane(k):
        return pltpu.make_async_remote_copy(
            src_ref=bias_sum, dst_ref=bias_plane.at[xy],
            send_sem=bplane_ssem.at[k], recv_sem=bplane_rsem.at[k],
            device_id=plane_peer(grp, tab, k), device_id_type=MESH,
        )

    def grad_to_plane(k):
        return pltpu.make_async_remote_copy(
            src_ref=plane_send.at[k], dst_ref=plane_recv.at[k],
            send_sem=plane_ssem.at[k], recv_sem=plane_rsem.at[k],
            device_id=plane_peer(grp, tab, k), device_id_type=MESH,
        )

    half_swap.wait()

    def fold(k):
        row = pl.multiple_of(flip(xy, k, 4) * 8, 8)
        wide = half_recv[pl.ds(flip(xy, k, 4), 1)][0].astype(jnp.float32)
        return grad[pl.ds(pl.multiple_of(mine + row, 8), 8), :] + wide

    def send_plane(k, _):
        plane_send[k] = fold(k).astype(jnp.bfloat16)
        grad_to_plane(k).start()
        bias_to_plane(k).start()
        return 0

    lax.fori_loop(1, 16, send_plane, 0)
    piece[...] = fold(0)

    def add_plane(k, _):
        grad_to_plane(k).wait_recv()
        bias_to_plane(k).wait_recv()
        piece[...] += plane_recv[k].astype(jnp.float32)
        return 0

    lax.fori_loop(1, 16, add_plane, 0)

    def grad_to_line(k):
        return pltpu.make_async_remote_copy(
            src_ref=line_send, dst_ref=line_recv.at[z],
            send_sem=line_ssem.at[k], recv_sem=line_rsem.at[k],
            device_id=column_peer(grp, tab, k), device_id_type=MESH,
        )

    line_send[...] = piece[...].astype(jnp.bfloat16)
    line_recv[pl.ds(z, 1)] = piece[...].astype(jnp.bfloat16)[None]
    for k in range(1, 8):
        grad_to_line(k).start()
    total = bias_plane[0]
    for k in range(1, 16):
        total = total + bias_plane[k]
    bias_sum_two[...] = total
    bias_line[pl.ds(z, 1)] = total[None]

    def bias_to_line(k):
        return pltpu.make_async_remote_copy(
            src_ref=bias_sum_two, dst_ref=bias_line.at[z],
            send_sem=bline_ssem.at[k], recv_sem=bline_rsem.at[k],
            device_id=column_peer(grp, tab, k), device_id_type=MESH,
        )

    for k in range(1, 8):
        bias_to_line(k).start()
    for k in range(1, 8):
        grad_to_line(k).wait_recv()
    block = line_recv[0].astype(jnp.float32)
    for k in range(1, 8):
        block = block + line_recv[k].astype(jnp.float32)
    plane_all[0] = block.astype(jnp.bfloat16)

    def block_to_plane(k):
        return pltpu.make_async_remote_copy(
            src_ref=plane_all.at[0], dst_ref=plane_all.at[k],
            send_sem=pall_ssem.at[k], recv_sem=pall_rsem.at[k],
            device_id=plane_peer(grp, tab, k), device_id_type=MESH,
        )

    def block_to_partner(k):
        return pltpu.make_async_remote_copy(
            src_ref=plane_all.at[k], dst_ref=half_all.at[k],
            send_sem=hall_ssem.at[k], recv_sem=hall_rsem.at[k],
            device_id=partner, device_id_type=MESH,
        )

    def start_blocks(k, _):
        block_to_plane(k).start()
        return 0

    lax.fori_loop(1, 16, start_blocks, 0)
    block_to_partner(0).start()
    for k in range(1, 8):
        bias_to_line(k).wait_recv()
    total = bias_line[0]
    for k in range(1, 8):
        total = total + bias_line[k]
    grad_bias_ref[...] = total

    def put(k, start, source):
        row = pl.multiple_of(start + flip(xy, k, 4) * 8, 8)
        grad_ref[pl.ds(row, 8), :] = source[k].astype(jnp.float32)

    put(0, mine, plane_all)

    def take_blocks(k, _):
        block_to_plane(k).wait_recv()
        block_to_partner(k).start()
        put(k, mine, plane_all)
        return 0

    lax.fori_loop(1, 16, take_blocks, 0)

    def take_halves(k, _):
        block_to_partner(k).wait_recv()
        put(k, other, half_all)
        block_to_partner(k).wait_send()
        return 0

    lax.fori_loop(0, 16, take_halves, 0)

    def finish_plane(k, _):
        grad_to_plane(k).wait_send()
        bias_to_plane(k).wait_send()
        block_to_plane(k).wait_send()
        return 0

    lax.fori_loop(1, 16, finish_plane, 0)
    for k in range(1, 8):
        grad_to_line(k).wait_send()
        bias_to_line(k).wait_send()

    def finish(offset, _):
        payload_copy(offset).wait_send()
        score_copy(offset).wait_send()
        return 0

    lax.fori_loop(1, peers, finish, 0)
    feature_copy(features_ref, Z_BIT).wait_send()

    def finish_features(m, _):
        feature_copy(features_ref, plane(m)).wait_send()
        passed_on(plane(m)).wait_send()
        return 0

    lax.fori_loop(1, PLANE, finish_features, 0)


def per_device(
    sample_ids, id_weights, dense_features, click_labels, table_shards, slot_table, top_weight, top_bias, out_weight,
):
    micro, local, columns = sample_ids.shape
    count = micro * local
    width = dense_features.shape[2]
    own_slots, vocab, _ = table_shards.shape
    tables, hidden_size = top_weight.shape
    peers = tables // own_slots
    samples_all = count * lax.axis_size("grp") * peers
    vmem, smem = pl.BlockSpec(memory_space=pltpu.VMEM), pl.BlockSpec(memory_space=pltpu.SMEM)
    anywhere = pl.BlockSpec(memory_space=pl.ANY)
    dma = pltpu.SemaphoreType.DMA
    bf16, f32 = jnp.bfloat16, jnp.float32

    logits, grad_top, grad_bias = pl.pallas_call(
        functools.partial(step_kernel, samples_all),
        out_shape=(
            jax.ShapeDtypeStruct((micro, local), f32),
            jax.ShapeDtypeStruct((tables, hidden_size), f32),
            jax.ShapeDtypeStruct((1, hidden_size), f32),
        ),
        in_specs=[smem] + [anywhere] * 9,
        out_specs=(vmem, vmem, vmem),
        scratch_shapes=[
            pltpu.VMEM((count, columns), jnp.int32),
            pltpu.VMEM((count, columns), bf16),
            pltpu.VMEM((count, width), bf16),
            pltpu.VMEM((own_slots, vocab, width), bf16),
            pltpu.VMEM((1, tables), jnp.int32),
            pltpu.VMEM((micro, local), jnp.int32),
            pltpu.VMEM((tables, hidden_size), bf16),
            pltpu.VMEM((1, hidden_size), f32),
            pltpu.VMEM((hidden_size,), bf16),
            pltpu.VMEM((tables, HOTS, count), f32),
            pltpu.VMEM((tables, HOTS, count), f32),
            pltpu.VMEM((peers, 2 * own_slots * HOTS, count), bf16),
            pltpu.VMEM((peers, 2 * own_slots * HOTS, count), bf16),
            pltpu.VMEM((peers, count, width), bf16),
            pltpu.VMEM((peers, own_slots, count), bf16),
            pltpu.VMEM((2, own_slots, count), f32),
            pltpu.VMEM((peers, own_slots, count), bf16),
            pltpu.VMEM((tables, hidden_size), f32),
            pltpu.VMEM((16, 8, hidden_size), bf16),
            pltpu.VMEM((16, 8, hidden_size), bf16),
            pltpu.VMEM((16, 8, hidden_size), bf16),
            pltpu.VMEM((16, 8, hidden_size), bf16),
            pltpu.VMEM((8, hidden_size), f32),
            pltpu.VMEM((8, hidden_size), bf16),
            pltpu.VMEM((8, 8, hidden_size), bf16),
            pltpu.VMEM((16, 8, hidden_size), bf16),
            pltpu.VMEM((16, 8, hidden_size), bf16),
            pltpu.VMEM((1, hidden_size), f32),
            pltpu.VMEM((1, hidden_size), f32),
            pltpu.VMEM((1, hidden_size), f32),
            pltpu.VMEM((16, 1, hidden_size), f32),
            pltpu.VMEM((1, hidden_size), f32),
            pltpu.VMEM((8, 1, hidden_size), f32),
            dma((9,)),
        ] + [dma((peers,)) for _ in range(6)] + [
            dma((2,)), dma((16,)), dma((16,)), dma((8,)), dma((8,)),
            dma((16,)), dma((16,)), dma((16,)), dma((16,)),
            dma((2,)), dma((16,)), dma((16,)), dma((8,)), dma((8,)),
        ],
        compiler_params=pltpu.CompilerParams(collective_id=0, has_side_effects=True, vmem_limit_bytes=60 << 20),
        name="step",
    )(
        slot_table,
        slot_table.reshape(1, tables),
        sample_ids.reshape(count, columns),
        id_weights.reshape(count, columns),
        dense_features.reshape(count, width),
        table_shards,
        click_labels,
        top_weight,
        top_bias.reshape(1, hidden_size),
        out_weight,
    )
    return logits, grad_top, grad_bias.reshape(hidden_size)


def solution(mesh):
    return jax.shard_map(
        per_device,
        mesh=mesh,
        in_specs=(
            P(None, ("grp", "tab"), None),
            P(None, ("grp", "tab"), None),
            P(None, ("grp", "tab"), None),
            P(None, ("grp", "tab")),
            P("tab", None, None),
            P(),
            P(),
            P(),
            P(),
        ),
        out_specs=(P(None, ("grp", "tab")), P(), P()),
        check_vma=False,
    )
```

```python
import functools
import math

import jax
import jax.numpy as jnp
from jax import lax
from jax.experimental import pallas as pl
from jax.experimental.pallas import tpu as pltpu
from jax.sharding import PartitionSpec as P

HOTS = 8
LANES = 128
MESH = pl.DeviceIdType.MESH
loss_scale = 32768.0

Z_BIT = 4
PLANE = 16
ROWS = 128
FIRST_NEAR = 10
FIRST_FAR = 4
FAR_RATE = 1
PASS_AT = 4


def place():
    grp, tab = lax.axis_index("grp"), lax.axis_index("tab")
    return grp, tab


def mirrored(grp):
    return (3 - grp // 2) * 2 + grp % 2


def plane(at):
    return (at // 4) * 8 + at % 4


def flip(value, offset, bits):
    total = 0
    for bit in range(bits):
        unit = 1 << bit
        one, two = (value // unit) % 2, (offset // unit) % 2
        total = total + (one + two - 2 * one * two) * unit
    return total


def peer_of(grp, tab, offset):
    cross = (offset // Z_BIT) % 2
    there = cross * mirrored(grp) + (1 - cross) * grp
    return {"grp": there, "tab": flip(tab, offset, 5)}


def gather_rows(source, index):
    dims = lax.GatherDimensionNumbers(
        offset_dims=(),
        collapsed_slice_dims=(0,),
        start_index_map=(0,),
        operand_batching_dims=(1,),
        start_indices_batching_dims=(1,),
    )
    return lax.gather(
        source, index[..., None], dims, slice_sizes=(1, 1),
        mode=lax.GatherScatterMode.PROMISE_IN_BOUNDS,
    )


def plane_peer(grp, tab, k):
    return {"grp": grp, "tab": flip(tab, (k // 4) * 8 + k % 4, 5)}


def column_peer(grp, tab, k):
    return {"grp": flip(grp, (k % 4) * 2, 3), "tab": flip(tab, (k // 4) * Z_BIT, 5)}


def step_kernel(
    samples_all,
    slots_ref, slots_hbm, ids_hbm, weights_hbm, features_hbm, tables_hbm, labels_hbm, top_hbm, bias_hbm, out_hbm,
    logits_ref, grad_ref, grad_bias_ref,
    ids_ref, weights_ref, features_ref, tables_ref, slot_row, labels_ref, top_ref, bias_ref, out_ref,
    ids_t, weights_t, send, recv, feats, back, summed, scores_ref,
    grad, half_send, half_recv, plane_send, plane_recv, piece, line_send, line_recv, plane_all, half_all,
    bias_part, bias_half, bias_sum, bias_plane, bias_sum_two, bias_line,
    load_sem, send_sem, recv_sem, fsend_sem, frecv_sem, bsend_sem, brecv_sem,
    half_sem, plane_ssem, plane_rsem, line_ssem, line_rsem, pall_ssem, pall_rsem, hall_ssem, hall_rsem,
    bhalf_sem, bplane_ssem, bplane_rsem, bline_ssem, bline_rsem,
):
    grp, tab = place()
    peers = send.shape[0]
    own_slots, vocab, width = tables_ref.shape
    lines = own_slots * HOTS
    loads = [
        pltpu.make_async_copy(source, target, load_sem.at[at])
        for at, (source, target) in enumerate(
            [
                (features_hbm, features_ref), (ids_hbm, ids_ref), (weights_hbm, weights_ref), (tables_hbm, tables_ref),
                (slots_hbm, slot_row), (labels_hbm, labels_ref), (top_hbm, top_ref), (bias_hbm, bias_ref), (out_hbm, out_ref),
            ]
        )
    ]
    for load in loads:
        load.start()
    barrier = pltpu.get_barrier_semaphore()

    def greet(offset, _):
        pl.semaphore_signal(barrier, inc=1, device_id=peer_of(grp, tab, offset), device_id_type=MESH)
        return 0

    def greet_column(k, _):
        pl.semaphore_signal(barrier, inc=1, device_id=column_peer(grp, tab, k), device_id_type=MESH)
        return 0

    partner = {"grp": flip(grp, 1, 3), "tab": tab}
    lax.fori_loop(1, peers, greet, 0)
    lax.fori_loop(1, 8, greet_column, 0)
    pl.semaphore_signal(barrier, inc=1, device_id=partner, device_id_type=MESH)
    loads[0].wait()
    feats[0] = features_ref[...]
    loads[1].wait()
    loads[2].wait()
    per_block = LANES // HOTS
    for at in range(ids_ref.shape[1] // LANES):
        columns = slice(at * LANES, (at + 1) * LANES)
        held = slice(at * per_block, (at + 1) * per_block)
        ids = ids_ref[:, columns]
        code = jnp.left_shift((ids & 127) + 128, jnp.right_shift(ids, 7))
        ids_t[held] = code.astype(jnp.float32).T.reshape(per_block, HOTS, LANES)
        weights_t[held] = weights_ref[:, columns].astype(jnp.float32).T.reshape(per_block, HOTS, LANES)

    def packed(offset, target):
        first = flip(tab, offset, 5) * own_slots
        for pair in range(own_slots // 2):
            one, two = slots_ref[first + 2 * pair], slots_ref[first + 2 * pair + 1]
            rows = slice(pair * 2 * HOTS, (pair + 1) * 2 * HOTS)
            target[offset, rows, :] = jnp.concatenate([ids_t[one], ids_t[two]], axis=0).astype(jnp.bfloat16)
            rows = slice(lines + pair * 2 * HOTS, lines + (pair + 1) * 2 * HOTS)
            target[offset, rows, :] = jnp.concatenate([weights_t[one], weights_t[two]], axis=0).astype(jnp.bfloat16)

    def pack_all(offset, _):
        packed(offset, send)
        return 0

    packed(0, recv)
    lax.fori_loop(1, peers, pack_all, 0)
    pl.semaphore_wait(barrier, peers - 1 + 7 + 1)

    def feature_copy(source, offset):
        return pltpu.make_async_remote_copy(
            src_ref=source, dst_ref=feats.at[offset],
            send_sem=fsend_sem.at[offset], recv_sem=frecv_sem.at[offset],
            device_id=peer_of(grp, tab, offset), device_id_type=MESH,
        )

    def passed_on(offset):
        return pltpu.make_async_remote_copy(
            src_ref=feats.at[Z_BIT], dst_ref=feats.at[offset + Z_BIT],
            send_sem=fsend_sem.at[offset + Z_BIT], recv_sem=frecv_sem.at[offset + Z_BIT],
            device_id=peer_of(grp, tab, offset), device_id_type=MESH,
        )

    def payload_copy(offset):
        return pltpu.make_async_remote_copy(
            src_ref=send.at[offset], dst_ref=recv.at[offset],
            send_sem=send_sem.at[offset], recv_sem=recv_sem.at[offset],
            device_id=peer_of(grp, tab, offset), device_id_type=MESH,
        )

    def score_copy(offset):
        return pltpu.make_async_remote_copy(
            src_ref=back.at[offset], dst_ref=scores_ref.at[tab],
            send_sem=bsend_sem.at[offset], recv_sem=brecv_sem.at[offset],
            device_id=peer_of(grp, tab, offset), device_id_type=MESH,
        )

    def send_near(at):
        offset = plane(at)
        feature_copy(features_ref, offset).start()
        payload_copy(offset).start()

    def send_far(at):
        offset = plane(at) + Z_BIT
        payload_copy(offset).start()

    def pass_features(at):
        passed_on(plane(at)).start()

    def first_near(at, _):
        send_near(at)
        return 0

    def first_far(at, _):
        send_far(at)
        return 0

    lax.fori_loop(1, FIRST_NEAR, first_near, 0)
    feature_copy(features_ref, Z_BIT).start()
    lax.fori_loop(0, FIRST_FAR, first_far, 0)

    def later_sends(m):
        for side in range(2):
            near = FIRST_NEAR + 2 * m + side

            @pl.when(near < PLANE)
            def _():
                send_near(near)

        for side in range(FAR_RATE):
            far = FIRST_FAR + FAR_RATE * m + side

            @pl.when(far < PLANE)
            def _():
                send_far(far)

        @pl.when(m == PASS_AT)
        def _():
            feature_copy(features_ref, Z_BIT).wait_recv()

        for side in range(2):
            place_to = 1 + 2 * (m - PASS_AT) + side

            @pl.when((m >= PASS_AT) & (place_to < PLANE))
            def _():
                pass_features(place_to)

    scale = 1.0 / math.sqrt(width)
    tile = 128

    loads[3].wait()

    def pair_step(m, _):
        both = [plane(2 * (m % 8) + side) + (m // 8) * Z_BIT for side in range(2)]

        @pl.when(m > 0)
        def _():
            payload_copy(both[0]).wait_recv()

        @pl.when(m % 8 > 0)
        def _():
            feature_copy(features_ref, both[0]).wait_recv()

        payload_copy(both[1]).wait_recv()
        feature_copy(features_ref, both[1]).wait_recv()
        later_sends(m)
        vectors = jnp.concatenate([feats[both[0]], feats[both[1]]], axis=0)

        for slot in range(own_slots):
            rows = slice(slot * HOTS, (slot + 1) * HOTS)
            low, chunk, total = [], [], []
            for source in both:
                code = recv[source, rows, :].astype(jnp.int32)
                high = jnp.zeros_like(code)
                for level in range(8, 8 + (vocab - 1) // 128):
                    high = high + (code >= (1 << level)).astype(jnp.int32)
                rest = jnp.right_shift(code, high) - 128
                low.append(rest & 7)
                chunk.append(high * 16 + jnp.right_shift(rest, 3))
                total.append(jnp.zeros((HOTS, LANES), jnp.float32))
            for part in range(vocab // tile):
                dots = lax.dot_general(
                    tables_ref[slot, part * tile : (part + 1) * tile, :], vectors,
                    (((1,), (1,)), ((), ())), preferred_element_type=jnp.float32,
                )
                for row in range(tile // HOTS):
                    at = part * (tile // HOTS) + row
                    for side in range(2):
                        found = gather_rows(
                            dots[row * HOTS : (row + 1) * HOTS, side * LANES : (side + 1) * LANES],
                            low[side],
                        )
                        total[side] = jnp.where(chunk[side] == at, found, total[side])
            weight_rows = slice(lines + slot * HOTS, lines + (slot + 1) * HOTS)
            for side, source in enumerate(both):
                weighed = total[side] * recv[source, weight_rows, :].astype(jnp.float32)
                summed[side, slot : slot + 1, :] = jnp.sum(weighed, axis=0, keepdims=True) * scale

        for side in range(2):
            back[both[side]] = summed[side].astype(jnp.bfloat16)

        @pl.when(m > 0)
        def _():
            score_copy(both[0]).start()

        score_copy(both[1]).start()

        return 0

    lax.fori_loop(0, PLANE, pair_step, 0)
    scores_ref[tab] = back[0]

    for load in loads[4:]:
        load.wait()

    def take_scores(offset, _):
        score_copy(offset).wait_recv()
        return 0

    lax.fori_loop(1, peers, take_scores, 0)

    core = grp % 2
    xy = (tab // 8) * 4 + tab % 4
    z = ((tab // Z_BIT) % 2) * 4 + grp // 2
    tables, hidden_size = top_ref.shape
    at_table = (lax.broadcasted_iota(jnp.int32, (tables, tables), 0) == slot_row[...]).astype(jnp.bfloat16)
    scores_wide = jnp.dot(at_table, scores_ref[...].reshape(tables, LANES), preferred_element_type=jnp.float32)
    scores_t = scores_wide.astype(jnp.bfloat16)
    scores = scores_wide.T.astype(jnp.bfloat16)
    pre = jnp.dot(scores, top_ref[...], preferred_element_type=jnp.float32) + bias_ref[...]
    gate = jax.nn.sigmoid(pre)
    hidden = (pre * gate).astype(jnp.bfloat16)
    out_wide = out_ref[...].astype(jnp.float32).reshape(1, hidden_size)
    logit_column = jnp.sum(hidden.astype(jnp.float32) * out_wide, axis=1, keepdims=True)
    micro, local = labels_ref.shape
    sample = lax.broadcasted_iota(jnp.int32, (LANES, local), 0)
    within = sample % local == lax.broadcasted_iota(jnp.int32, (LANES, local), 1)
    batch_of = lax.broadcasted_iota(jnp.int32, (LANES, micro), 0) // local
    spread = lax.dot_general(
        within.astype(jnp.float32), labels_ref[...].astype(jnp.float32),
        (((1,), (1,)), ((), ())), preferred_element_type=jnp.float32,
    )
    own_batch = batch_of == lax.broadcasted_iota(jnp.int32, (LANES, micro), 1)
    labels = jnp.sum(jnp.where(own_batch, spread, 0.0), axis=1, keepdims=True)
    rows_of = lax.broadcasted_iota(jnp.int32, (micro, LANES), 1) // local
    picks = (rows_of == lax.broadcasted_iota(jnp.int32, (micro, LANES), 0)).astype(jnp.float32)
    logits_ref[...] = jnp.dot(
        picks, jnp.where(within, logit_column, 0.0),
        precision=lax.Precision.HIGHEST, preferred_element_type=jnp.float32,
    )
    delta = (jax.nn.sigmoid(logit_column) - labels) * (loss_scale / samples_all)
    slope = gate * (1.0 + pre * (1.0 - gate))
    hidden_grad_wide = delta * out_wide * slope
    hidden_grad = hidden_grad_wide.astype(jnp.bfloat16)
    grad[...] = jnp.dot(scores_t, hidden_grad, preferred_element_type=jnp.float32)
    bias_part[...] = jnp.sum(hidden_grad.astype(jnp.float32), axis=0, keepdims=True)

    other = pl.multiple_of((1 - core) * ROWS, ROWS)
    mine = pl.multiple_of(core * ROWS, ROWS)
    half_send[...] = grad[pl.ds(other, ROWS), :].reshape(16, 8, hidden_size).astype(jnp.bfloat16)

    def to_partner(source, target, sems):
        return pltpu.make_async_remote_copy(
            src_ref=source, dst_ref=target, send_sem=sems.at[0], recv_sem=sems.at[1],
            device_id=partner, device_id_type=MESH,
        )

    bias_swap = to_partner(bias_part, bias_half, bhalf_sem)
    half_swap = to_partner(half_send, half_recv, half_sem)
    bias_swap.start()
    half_swap.start()
    bias_swap.wait()
    bias_sum[...] = bias_part[...] + bias_half[...]
    bias_plane[pl.ds(xy, 1)] = bias_sum[...][None]

    def bias_to_plane(k):
        return pltpu.make_async_remote_copy(
            src_ref=bias_sum, dst_ref=bias_plane.at[xy],
            send_sem=bplane_ssem.at[k], recv_sem=bplane_rsem.at[k],
            device_id=plane_peer(grp, tab, k), device_id_type=MESH,
        )

    def grad_to_plane(k):
        return pltpu.make_async_remote_copy(
            src_ref=plane_send.at[k], dst_ref=plane_recv.at[k],
            send_sem=plane_ssem.at[k], recv_sem=plane_rsem.at[k],
            device_id=plane_peer(grp, tab, k), device_id_type=MESH,
        )

    half_swap.wait()

    def fold(k):
        row = pl.multiple_of(flip(xy, k, 4) * 8, 8)
        wide = half_recv[pl.ds(flip(xy, k, 4), 1)][0].astype(jnp.float32)
        return grad[pl.ds(pl.multiple_of(mine + row, 8), 8), :] + wide

    def send_plane(k, _):
        plane_send[k] = fold(k).astype(jnp.bfloat16)
        grad_to_plane(k).start()
        bias_to_plane(k).start()
        return 0

    lax.fori_loop(1, 16, send_plane, 0)
    piece[...] = fold(0)

    def add_plane(k, _):
        grad_to_plane(k).wait_recv()
        bias_to_plane(k).wait_recv()
        piece[...] += plane_recv[k].astype(jnp.float32)
        return 0

    lax.fori_loop(1, 16, add_plane, 0)

    def grad_to_line(k):
        return pltpu.make_async_remote_copy(
            src_ref=line_send, dst_ref=line_recv.at[z],
            send_sem=line_ssem.at[k], recv_sem=line_rsem.at[k],
            device_id=column_peer(grp, tab, k), device_id_type=MESH,
        )

    line_send[...] = piece[...].astype(jnp.bfloat16)
    line_recv[pl.ds(z, 1)] = piece[...].astype(jnp.bfloat16)[None]
    for k in range(1, 8):
        grad_to_line(k).start()
    total = bias_plane[0]
    for k in range(1, 16):
        total = total + bias_plane[k]
    bias_sum_two[...] = total
    bias_line[pl.ds(z, 1)] = total[None]

    def bias_to_line(k):
        return pltpu.make_async_remote_copy(
            src_ref=bias_sum_two, dst_ref=bias_line.at[z],
            send_sem=bline_ssem.at[k], recv_sem=bline_rsem.at[k],
            device_id=column_peer(grp, tab, k), device_id_type=MESH,
        )

    for k in range(1, 8):
        bias_to_line(k).start()
    for k in range(1, 8):
        grad_to_line(k).wait_recv()
    block = line_recv[0].astype(jnp.float32)
    for k in range(1, 8):
        block = block + line_recv[k].astype(jnp.float32)
    plane_all[0] = block.astype(jnp.bfloat16)

    def block_to_plane(k):
        return pltpu.make_async_remote_copy(
            src_ref=plane_all.at[0], dst_ref=plane_all.at[k],
            send_sem=pall_ssem.at[k], recv_sem=pall_rsem.at[k],
            device_id=plane_peer(grp, tab, k), device_id_type=MESH,
        )

    def block_to_partner(k):
        return pltpu.make_async_remote_copy(
            src_ref=plane_all.at[k], dst_ref=half_all.at[k],
            send_sem=hall_ssem.at[k], recv_sem=hall_rsem.at[k],
            device_id=partner, device_id_type=MESH,
        )

    def start_blocks(k, _):
        block_to_plane(k).start()
        return 0

    lax.fori_loop(1, 16, start_blocks, 0)
    block_to_partner(0).start()
    for k in range(1, 8):
        bias_to_line(k).wait_recv()
    total = bias_line[0]
    for k in range(1, 8):
        total = total + bias_line[k]
    grad_bias_ref[...] = total

    def put(k, start, source):
        row = pl.multiple_of(start + flip(xy, k, 4) * 8, 8)
        grad_ref[pl.ds(row, 8), :] = source[k].astype(jnp.float32)

    put(0, mine, plane_all)

    def take_blocks(k, _):
        block_to_plane(k).wait_recv()
        block_to_partner(k).start()
        put(k, mine, plane_all)
        return 0

    lax.fori_loop(1, 16, take_blocks, 0)

    def take_halves(k, _):
        block_to_partner(k).wait_recv()
        put(k, other, half_all)
        block_to_partner(k).wait_send()
        return 0

    lax.fori_loop(0, 16, take_halves, 0)

    def finish_plane(k, _):
        grad_to_plane(k).wait_send()
        bias_to_plane(k).wait_send()
        block_to_plane(k).wait_send()
        return 0

    lax.fori_loop(1, 16, finish_plane, 0)
    for k in range(1, 8):
        grad_to_line(k).wait_send()
        bias_to_line(k).wait_send()

    def finish(offset, _):
        payload_copy(offset).wait_send()
        score_copy(offset).wait_send()
        return 0

    lax.fori_loop(1, peers, finish, 0)
    feature_copy(features_ref, Z_BIT).wait_send()

    def finish_features(m, _):
        feature_copy(features_ref, plane(m)).wait_send()
        passed_on(plane(m)).wait_send()
        return 0

    lax.fori_loop(1, PLANE, finish_features, 0)


def per_device(
    sample_ids, id_weights, dense_features, click_labels, table_shards, slot_table, top_weight, top_bias, out_weight,
):
    micro, local, columns = sample_ids.shape
    count = micro * local
    width = dense_features.shape[2]
    own_slots, vocab, _ = table_shards.shape
    tables, hidden_size = top_weight.shape
    peers = tables // own_slots
    samples_all = count * lax.axis_size("grp") * peers
    vmem, smem = pl.BlockSpec(memory_space=pltpu.VMEM), pl.BlockSpec(memory_space=pltpu.SMEM)
    anywhere = pl.BlockSpec(memory_space=pl.ANY)
    dma = pltpu.SemaphoreType.DMA
    bf16, f32 = jnp.bfloat16, jnp.float32

    logits, grad_top, grad_bias = pl.pallas_call(
        functools.partial(step_kernel, samples_all),
        out_shape=(
            jax.ShapeDtypeStruct((micro, local), f32),
            jax.ShapeDtypeStruct((tables, hidden_size), f32),
            jax.ShapeDtypeStruct((1, hidden_size), f32),
        ),
        in_specs=[smem] + [anywhere] * 9,
        out_specs=(vmem, vmem, vmem),
        scratch_shapes=[
            pltpu.VMEM((count, columns), jnp.int32),
            pltpu.VMEM((count, columns), bf16),
            pltpu.VMEM((count, width), bf16),
            pltpu.VMEM((own_slots, vocab, width), bf16),
            pltpu.VMEM((1, tables), jnp.int32),
            pltpu.VMEM((micro, local), jnp.int32),
            pltpu.VMEM((tables, hidden_size), bf16),
            pltpu.VMEM((1, hidden_size), f32),
            pltpu.VMEM((hidden_size,), bf16),
            pltpu.VMEM((tables, HOTS, count), f32),
            pltpu.VMEM((tables, HOTS, count), f32),
            pltpu.VMEM((peers, 2 * own_slots * HOTS, count), bf16),
            pltpu.VMEM((peers, 2 * own_slots * HOTS, count), bf16),
            pltpu.VMEM((peers, count, width), bf16),
            pltpu.VMEM((peers, own_slots, count), bf16),
            pltpu.VMEM((2, own_slots, count), f32),
            pltpu.VMEM((peers, own_slots, count), bf16),
            pltpu.VMEM((tables, hidden_size), f32),
            pltpu.VMEM((16, 8, hidden_size), bf16),
            pltpu.VMEM((16, 8, hidden_size), bf16),
            pltpu.VMEM((16, 8, hidden_size), bf16),
            pltpu.VMEM((16, 8, hidden_size), bf16),
            pltpu.VMEM((8, hidden_size), f32),
            pltpu.VMEM((8, hidden_size), bf16),
            pltpu.VMEM((8, 8, hidden_size), bf16),
            pltpu.VMEM((16, 8, hidden_size), bf16),
            pltpu.VMEM((16, 8, hidden_size), bf16),
            pltpu.VMEM((1, hidden_size), f32),
            pltpu.VMEM((1, hidden_size), f32),
            pltpu.VMEM((1, hidden_size), f32),
            pltpu.VMEM((16, 1, hidden_size), f32),
            pltpu.VMEM((1, hidden_size), f32),
            pltpu.VMEM((8, 1, hidden_size), f32),
            dma((9,)),
        ] + [dma((peers,)) for _ in range(6)] + [
            dma((2,)), dma((16,)), dma((16,)), dma((8,)), dma((8,)),
            dma((16,)), dma((16,)), dma((16,)), dma((16,)),
            dma((2,)), dma((16,)), dma((16,)), dma((8,)), dma((8,)),
        ],
        compiler_params=pltpu.CompilerParams(collective_id=0, has_side_effects=True, vmem_limit_bytes=60 << 20),
        name="step",
    )(
        slot_table,
        slot_table.reshape(1, tables),
        sample_ids.reshape(count, columns),
        id_weights.reshape(count, columns),
        dense_features.reshape(count, width),
        table_shards,
        click_labels,
        top_weight,
        top_bias.reshape(1, hidden_size),
        out_weight,
    )
    return logits, grad_top, grad_bias.reshape(hidden_size)


def solution(mesh):
    return jax.shard_map(
        per_device,
        mesh=mesh,
        in_specs=(
            P(None, ("grp", "tab"), None),
            P(None, ("grp", "tab"), None),
            P(None, ("grp", "tab"), None),
            P(None, ("grp", "tab")),
            P("tab", None, None),
            P(),
            P(),
            P(),
            P(),
        ),
        out_specs=(P(None, ("grp", "tab")), P(), P()),
        check_vma=False,
    )
```

```python
import functools
import math

import jax
import jax.numpy as jnp
from jax import lax
from jax.experimental import pallas as pl
from jax.experimental.pallas import tpu as pltpu
from jax.sharding import PartitionSpec as P

HOTS = 8
LANES = 128
MESH = pl.DeviceIdType.MESH
loss_scale = 32768.0

Z_BIT = 4
PLANE = 16
ROWS = 128
FIRST_NEAR = 8
FIRST_FAR = 4
FAR_RATE = 1
PASS_AT = 4


def place():
    grp, tab = lax.axis_index("grp"), lax.axis_index("tab")
    return grp, tab


def mirrored(grp):
    return (3 - grp // 2) * 2 + grp % 2


def plane(at):
    return (at // 4) * 8 + at % 4


def flip(value, offset, bits):
    total = 0
    for bit in range(bits):
        unit = 1 << bit
        one, two = (value // unit) % 2, (offset // unit) % 2
        total = total + (one + two - 2 * one * two) * unit
    return total


def peer_of(grp, tab, offset):
    cross = (offset // Z_BIT) % 2
    there = cross * mirrored(grp) + (1 - cross) * grp
    return {"grp": there, "tab": flip(tab, offset, 5)}


def gather_rows(source, index):
    dims = lax.GatherDimensionNumbers(
        offset_dims=(),
        collapsed_slice_dims=(0,),
        start_index_map=(0,),
        operand_batching_dims=(1,),
        start_indices_batching_dims=(1,),
    )
    return lax.gather(
        source, index[..., None], dims, slice_sizes=(1, 1),
        mode=lax.GatherScatterMode.PROMISE_IN_BOUNDS,
    )


def plane_peer(grp, tab, k):
    return {"grp": grp, "tab": flip(tab, (k // 4) * 8 + k % 4, 5)}


def column_peer(grp, tab, k):
    return {"grp": flip(grp, (k % 4) * 2, 3), "tab": flip(tab, (k // 4) * Z_BIT, 5)}


def step_kernel(
    samples_all,
    slots_ref, slots_hbm, ids_hbm, weights_hbm, features_hbm, tables_hbm, labels_hbm, top_hbm, bias_hbm, out_hbm,
    logits_ref, grad_ref, grad_bias_ref,
    ids_ref, weights_ref, features_ref, tables_ref, slot_row, labels_ref, top_ref, bias_ref, out_ref,
    ids_t, weights_t, send, recv, feats, back, summed, scores_ref,
    grad, half_send, half_recv, plane_send, plane_recv, piece, line_send, line_recv, plane_all, half_all,
    bias_part, bias_half, bias_sum, bias_plane, bias_sum_two, bias_line,
    load_sem, send_sem, recv_sem, fsend_sem, frecv_sem, bsend_sem, brecv_sem,
    half_sem, plane_ssem, plane_rsem, line_ssem, line_rsem, pall_ssem, pall_rsem, hall_ssem, hall_rsem,
    bhalf_sem, bplane_ssem, bplane_rsem, bline_ssem, bline_rsem,
):
    grp, tab = place()
    peers = send.shape[0]
    own_slots, vocab, width = tables_ref.shape
    lines = own_slots * HOTS
    loads = [
        pltpu.make_async_copy(source, target, load_sem.at[at])
        for at, (source, target) in enumerate(
            [
                (features_hbm, features_ref), (ids_hbm, ids_ref), (weights_hbm, weights_ref), (tables_hbm, tables_ref),
                (slots_hbm, slot_row), (labels_hbm, labels_ref), (top_hbm, top_ref), (bias_hbm, bias_ref), (out_hbm, out_ref),
            ]
        )
    ]
    for load in loads:
        load.start()
    barrier = pltpu.get_barrier_semaphore()

    def greet(offset, _):
        pl.semaphore_signal(barrier, inc=1, device_id=peer_of(grp, tab, offset), device_id_type=MESH)
        return 0

    def greet_column(k, _):
        pl.semaphore_signal(barrier, inc=1, device_id=column_peer(grp, tab, k), device_id_type=MESH)
        return 0

    partner = {"grp": flip(grp, 1, 3), "tab": tab}
    lax.fori_loop(1, peers, greet, 0)
    lax.fori_loop(1, 8, greet_column, 0)
    pl.semaphore_signal(barrier, inc=1, device_id=partner, device_id_type=MESH)
    loads[0].wait()
    feats[0] = features_ref[...]
    loads[1].wait()
    loads[2].wait()
    per_block = LANES // HOTS
    for at in range(ids_ref.shape[1] // LANES):
        columns = slice(at * LANES, (at + 1) * LANES)
        held = slice(at * per_block, (at + 1) * per_block)
        ids = ids_ref[:, columns]
        code = jnp.left_shift((ids & 127) + 128, jnp.right_shift(ids, 7))
        ids_t[held] = code.astype(jnp.float32).T.reshape(per_block, HOTS, LANES)
        weights_t[held] = weights_ref[:, columns].astype(jnp.float32).T.reshape(per_block, HOTS, LANES)

    def packed(offset, target):
        first = flip(tab, offset, 5) * own_slots
        for pair in range(own_slots // 2):
            one, two = slots_ref[first + 2 * pair], slots_ref[first + 2 * pair + 1]
            rows = slice(pair * 2 * HOTS, (pair + 1) * 2 * HOTS)
            target[offset, rows, :] = jnp.concatenate([ids_t[one], ids_t[two]], axis=0).astype(jnp.bfloat16)
            rows = slice(lines + pair * 2 * HOTS, lines + (pair + 1) * 2 * HOTS)
            target[offset, rows, :] = jnp.concatenate([weights_t[one], weights_t[two]], axis=0).astype(jnp.bfloat16)

    def pack_all(offset, _):
        packed(offset, send)
        return 0

    packed(0, recv)
    lax.fori_loop(1, peers, pack_all, 0)
    pl.semaphore_wait(barrier, peers - 1 + 7 + 1)

    def feature_copy(source, offset):
        return pltpu.make_async_remote_copy(
            src_ref=source, dst_ref=feats.at[offset],
            send_sem=fsend_sem.at[offset], recv_sem=frecv_sem.at[offset],
            device_id=peer_of(grp, tab, offset), device_id_type=MESH,
        )

    def passed_on(offset):
        return pltpu.make_async_remote_copy(
            src_ref=feats.at[Z_BIT], dst_ref=feats.at[offset + Z_BIT],
            send_sem=fsend_sem.at[offset + Z_BIT], recv_sem=frecv_sem.at[offset + Z_BIT],
            device_id=peer_of(grp, tab, offset), device_id_type=MESH,
        )

    def payload_copy(offset):
        return pltpu.make_async_remote_copy(
            src_ref=send.at[offset], dst_ref=recv.at[offset],
            send_sem=send_sem.at[offset], recv_sem=recv_sem.at[offset],
            device_id=peer_of(grp, tab, offset), device_id_type=MESH,
        )

    def score_copy(offset):
        return pltpu.make_async_remote_copy(
            src_ref=back.at[offset], dst_ref=scores_ref.at[tab],
            send_sem=bsend_sem.at[offset], recv_sem=brecv_sem.at[offset],
            device_id=peer_of(grp, tab, offset), device_id_type=MESH,
        )

    feature_copy(features_ref, Z_BIT).start()

    def send_near(at):
        offset = plane(at)
        feature_copy(features_ref, offset).start()
        payload_copy(offset).start()

    def send_far(at):
        offset = plane(at) + Z_BIT
        payload_copy(offset).start()

    def pass_features(at):
        passed_on(plane(at)).start()

    def first_sends(at, _):
        @pl.when(at < FIRST_NEAR)
        def _():
            send_near(at)

        @pl.when(at - 1 < FIRST_FAR)
        def _():
            send_far(at - 1)

        return 0

    lax.fori_loop(1, max(FIRST_NEAR, FIRST_FAR + 1), first_sends, 0)

    def later_sends(m):
        for side in range(2):
            near = FIRST_NEAR + 2 * m + side

            @pl.when(near < PLANE)
            def _():
                send_near(near)

        for side in range(FAR_RATE):
            far = FIRST_FAR + FAR_RATE * m + side

            @pl.when(far < PLANE)
            def _():
                send_far(far)

        @pl.when(m == PASS_AT)
        def _():
            feature_copy(features_ref, Z_BIT).wait_recv()

        for side in range(2):
            place_to = 1 + 2 * (m - PASS_AT) + side

            @pl.when((m >= PASS_AT) & (place_to < PLANE))
            def _():
                pass_features(place_to)

    scale = 1.0 / math.sqrt(width)
    tile = 128

    loads[3].wait()

    def pair_step(m, _):
        both = [plane(2 * (m % 8) + side) + (m // 8) * Z_BIT for side in range(2)]

        @pl.when(m > 0)
        def _():
            payload_copy(both[0]).wait_recv()

        @pl.when(m % 8 > 0)
        def _():
            feature_copy(features_ref, both[0]).wait_recv()

        payload_copy(both[1]).wait_recv()
        feature_copy(features_ref, both[1]).wait_recv()
        later_sends(m)
        vectors = jnp.concatenate([feats[both[0]], feats[both[1]]], axis=0)

        for slot in range(own_slots):
            rows = slice(slot * HOTS, (slot + 1) * HOTS)
            low, chunk, total = [], [], []
            for source in both:
                code = recv[source, rows, :].astype(jnp.int32)
                high = jnp.zeros_like(code)
                for level in range(8, 8 + (vocab - 1) // 128):
                    high = high + (code >= (1 << level)).astype(jnp.int32)
                rest = jnp.right_shift(code, high) - 128
                low.append(rest & 7)
                chunk.append(high * 16 + jnp.right_shift(rest, 3))
                total.append(jnp.zeros((HOTS, LANES), jnp.float32))
            for part in range(vocab // tile):
                dots = lax.dot_general(
                    tables_ref[slot, part * tile : (part + 1) * tile, :], vectors,
                    (((1,), (1,)), ((), ())), preferred_element_type=jnp.float32,
                )
                for row in range(tile // HOTS):
                    at = part * (tile // HOTS) + row
                    for side in range(2):
                        found = gather_rows(
                            dots[row * HOTS : (row + 1) * HOTS, side * LANES : (side + 1) * LANES],
                            low[side],
                        )
                        total[side] = jnp.where(chunk[side] == at, found, total[side])
            weight_rows = slice(lines + slot * HOTS, lines + (slot + 1) * HOTS)
            for side, source in enumerate(both):
                weighed = total[side] * recv[source, weight_rows, :].astype(jnp.float32)
                summed[side, slot : slot + 1, :] = jnp.sum(weighed, axis=0, keepdims=True) * scale

        for side in range(2):
            back[both[side]] = summed[side].astype(jnp.bfloat16)

        @pl.when(m > 0)
        def _():
            score_copy(both[0]).start()

        score_copy(both[1]).start()

        return 0

    lax.fori_loop(0, PLANE, pair_step, 0)
    scores_ref[tab] = back[0]

    for load in loads[4:]:
        load.wait()

    micro, local = labels_ref.shape
    sample = lax.broadcasted_iota(jnp.int32, (LANES, local), 0)
    within = sample % local == lax.broadcasted_iota(jnp.int32, (LANES, local), 1)
    batch_of = lax.broadcasted_iota(jnp.int32, (LANES, micro), 0) // local
    spread = lax.dot_general(
        within.astype(jnp.float32), labels_ref[...].astype(jnp.float32),
        (((1,), (1,)), ((), ())), preferred_element_type=jnp.float32,
    )
    own_batch = batch_of == lax.broadcasted_iota(jnp.int32, (LANES, micro), 1)
    labels = jnp.sum(jnp.where(own_batch, spread, 0.0), axis=1, keepdims=True)

    def take_scores(offset, _):
        score_copy(offset).wait_recv()
        return 0

    lax.fori_loop(1, peers, take_scores, 0)

    core = grp % 2
    xy = (tab // 8) * 4 + tab % 4
    z = ((tab // Z_BIT) % 2) * 4 + grp // 2
    tables, hidden_size = top_ref.shape
    at_table = (lax.broadcasted_iota(jnp.int32, (tables, tables), 0) == slot_row[...]).astype(jnp.bfloat16)
    scores_wide = jnp.dot(at_table, scores_ref[...].reshape(tables, LANES), preferred_element_type=jnp.float32)
    scores = scores_wide.T.astype(jnp.bfloat16)
    pre = jnp.dot(scores, top_ref[...], preferred_element_type=jnp.float32) + bias_ref[...]
    gate = jax.nn.sigmoid(pre)
    hidden = (pre * gate).astype(jnp.bfloat16)
    out_wide = out_ref[...].astype(jnp.float32).reshape(1, hidden_size)
    logit_column = jnp.sum(hidden.astype(jnp.float32) * out_wide, axis=1, keepdims=True)
    delta = (jax.nn.sigmoid(logit_column) - labels) * (loss_scale / samples_all)
    slope = gate * (1.0 + pre * (1.0 - gate))
    hidden_grad_wide = delta * out_wide * slope
    hidden_grad = hidden_grad_wide.astype(jnp.bfloat16)
    other = pl.multiple_of((1 - core) * ROWS, ROWS)
    mine = pl.multiple_of(core * ROWS, ROWS)

    def to_partner(source, target, sems):
        return pltpu.make_async_remote_copy(
            src_ref=source, dst_ref=target, send_sem=sems.at[0], recv_sem=sems.at[1],
            device_id=partner, device_id_type=MESH,
        )

    def half_grad(start):
        at = lax.broadcasted_iota(jnp.int32, (ROWS, tables), 0) + start == slot_row[...]
        rows = jnp.dot(
            at.astype(jnp.bfloat16), scores_ref[...].reshape(tables, LANES), preferred_element_type=jnp.float32
        ).astype(jnp.bfloat16)
        return jnp.dot(rows, hidden_grad, preferred_element_type=jnp.float32)

    bias_swap = to_partner(bias_part, bias_half, bhalf_sem)
    half_swap = to_partner(half_send, half_recv, half_sem)
    bias_part[...] = jnp.sum(hidden_grad.astype(jnp.float32), axis=0, keepdims=True)
    bias_swap.start()
    half_send[...] = half_grad(other).reshape(16, 8, hidden_size).astype(jnp.bfloat16)
    half_swap.start()
    grad[...] = half_grad(mine)
    rows_of = lax.broadcasted_iota(jnp.int32, (micro, LANES), 1) // local
    picks = (rows_of == lax.broadcasted_iota(jnp.int32, (micro, LANES), 0)).astype(jnp.float32)
    logits_ref[...] = jnp.dot(
        picks, jnp.where(within, logit_column, 0.0),
        precision=lax.Precision.HIGHEST, preferred_element_type=jnp.float32,
    )
    bias_swap.wait()
    bias_sum[...] = bias_part[...] + bias_half[...]
    bias_plane[pl.ds(xy, 1)] = bias_sum[...][None]

    def bias_to_plane(k):
        return pltpu.make_async_remote_copy(
            src_ref=bias_sum, dst_ref=bias_plane.at[xy],
            send_sem=bplane_ssem.at[k], recv_sem=bplane_rsem.at[k],
            device_id=plane_peer(grp, tab, k), device_id_type=MESH,
        )

    def grad_to_plane(k):
        return pltpu.make_async_remote_copy(
            src_ref=plane_send.at[k], dst_ref=plane_recv.at[k],
            send_sem=plane_ssem.at[k], recv_sem=plane_rsem.at[k],
            device_id=plane_peer(grp, tab, k), device_id_type=MESH,
        )

    half_swap.wait()

    def fold(k):
        row = pl.multiple_of(flip(xy, k, 4) * 8, 8)
        wide = half_recv[pl.ds(flip(xy, k, 4), 1)][0].astype(jnp.float32)
        return grad[pl.ds(row, 8), :] + wide

    def send_plane(k, _):
        plane_send[k] = fold(k).astype(jnp.bfloat16)
        grad_to_plane(k).start()
        bias_to_plane(k).start()
        return 0

    lax.fori_loop(1, 16, send_plane, 0)
    piece[...] = fold(0)

    def add_plane(k, _):
        grad_to_plane(k).wait_recv()
        bias_to_plane(k).wait_recv()
        piece[...] += plane_recv[k].astype(jnp.float32)
        return 0

    lax.fori_loop(1, 16, add_plane, 0)

    def grad_to_line(k):
        return pltpu.make_async_remote_copy(
            src_ref=line_send, dst_ref=line_recv.at[z],
            send_sem=line_ssem.at[k], recv_sem=line_rsem.at[k],
            device_id=column_peer(grp, tab, k), device_id_type=MESH,
        )

    line_send[...] = piece[...].astype(jnp.bfloat16)
    line_recv[pl.ds(z, 1)] = piece[...].astype(jnp.bfloat16)[None]
    for k in range(1, 8):
        grad_to_line(k).start()
    total = bias_plane[0]
    for k in range(1, 16):
        total = total + bias_plane[k]
    bias_sum_two[...] = total
    bias_line[pl.ds(z, 1)] = total[None]

    def bias_to_line(k):
        return pltpu.make_async_remote_copy(
            src_ref=bias_sum_two, dst_ref=bias_line.at[z],
            send_sem=bline_ssem.at[k], recv_sem=bline_rsem.at[k],
            device_id=column_peer(grp, tab, k), device_id_type=MESH,
        )

    for k in range(1, 8):
        bias_to_line(k).start()
    for k in range(1, 8):
        grad_to_line(k).wait_recv()
    block = line_recv[0].astype(jnp.float32)
    for k in range(1, 8):
        block = block + line_recv[k].astype(jnp.float32)
    plane_all[0] = block.astype(jnp.bfloat16)

    def block_to_plane(k):
        return pltpu.make_async_remote_copy(
            src_ref=plane_all.at[0], dst_ref=plane_all.at[k],
            send_sem=pall_ssem.at[k], recv_sem=pall_rsem.at[k],
            device_id=plane_peer(grp, tab, k), device_id_type=MESH,
        )

    def block_to_partner(k):
        return pltpu.make_async_remote_copy(
            src_ref=plane_all.at[k], dst_ref=half_all.at[k],
            send_sem=hall_ssem.at[k], recv_sem=hall_rsem.at[k],
            device_id=partner, device_id_type=MESH,
        )

    def start_blocks(k, _):
        block_to_plane(k).start()
        return 0

    lax.fori_loop(1, 16, start_blocks, 0)
    block_to_partner(0).start()
    for k in range(1, 8):
        bias_to_line(k).wait_recv()
    total = bias_line[0]
    for k in range(1, 8):
        total = total + bias_line[k]
    grad_bias_ref[...] = total

    def put(k, start, source):
        row = pl.multiple_of(start + flip(xy, k, 4) * 8, 8)
        grad_ref[pl.ds(row, 8), :] = source[k].astype(jnp.float32)

    put(0, mine, plane_all)

    def take_blocks(k, _):
        block_to_plane(k).wait_recv()
        block_to_partner(k).start()
        put(k, mine, plane_all)
        return 0

    lax.fori_loop(1, 16, take_blocks, 0)

    def take_halves(k, _):
        block_to_partner(k).wait_recv()
        put(k, other, half_all)
        block_to_partner(k).wait_send()
        return 0

    lax.fori_loop(0, 16, take_halves, 0)

    def finish_plane(k, _):
        grad_to_plane(k).wait_send()
        bias_to_plane(k).wait_send()
        block_to_plane(k).wait_send()
        return 0

    lax.fori_loop(1, 16, finish_plane, 0)
    for k in range(1, 8):
        grad_to_line(k).wait_send()
        bias_to_line(k).wait_send()

    def finish(offset, _):
        payload_copy(offset).wait_send()
        score_copy(offset).wait_send()
        return 0

    lax.fori_loop(1, peers, finish, 0)
    feature_copy(features_ref, Z_BIT).wait_send()

    def finish_features(m, _):
        feature_copy(features_ref, plane(m)).wait_send()
        passed_on(plane(m)).wait_send()
        return 0

    lax.fori_loop(1, PLANE, finish_features, 0)


def per_device(
    sample_ids, id_weights, dense_features, click_labels, table_shards, slot_table, top_weight, top_bias, out_weight,
):
    micro, local, columns = sample_ids.shape
    count = micro * local
    width = dense_features.shape[2]
    own_slots, vocab, _ = table_shards.shape
    tables, hidden_size = top_weight.shape
    peers = tables // own_slots
    samples_all = count * lax.axis_size("grp") * peers
    vmem, smem = pl.BlockSpec(memory_space=pltpu.VMEM), pl.BlockSpec(memory_space=pltpu.SMEM)
    anywhere = pl.BlockSpec(memory_space=pl.ANY)
    dma = pltpu.SemaphoreType.DMA
    bf16, f32 = jnp.bfloat16, jnp.float32

    logits, grad_top, grad_bias = pl.pallas_call(
        functools.partial(step_kernel, samples_all),
        out_shape=(
            jax.ShapeDtypeStruct((micro, local), f32),
            jax.ShapeDtypeStruct((tables, hidden_size), f32),
            jax.ShapeDtypeStruct((1, hidden_size), f32),
        ),
        in_specs=[smem] + [anywhere] * 9,
        out_specs=(vmem, vmem, vmem),
        scratch_shapes=[
            pltpu.VMEM((count, columns), jnp.int32),
            pltpu.VMEM((count, columns), bf16),
            pltpu.VMEM((count, width), bf16),
            pltpu.VMEM((own_slots, vocab, width), bf16),
            pltpu.VMEM((1, tables), jnp.int32),
            pltpu.VMEM((micro, local), jnp.int32),
            pltpu.VMEM((tables, hidden_size), bf16),
            pltpu.VMEM((1, hidden_size), f32),
            pltpu.VMEM((hidden_size,), bf16),
            pltpu.VMEM((tables, HOTS, count), f32),
            pltpu.VMEM((tables, HOTS, count), f32),
            pltpu.VMEM((peers, 2 * own_slots * HOTS, count), bf16),
            pltpu.VMEM((peers, 2 * own_slots * HOTS, count), bf16),
            pltpu.VMEM((peers, count, width), bf16),
            pltpu.VMEM((peers, own_slots, count), bf16),
            pltpu.VMEM((2, own_slots, count), f32),
            pltpu.VMEM((peers, own_slots, count), bf16),
            pltpu.VMEM((ROWS, hidden_size), f32),
            pltpu.VMEM((16, 8, hidden_size), bf16),
            pltpu.VMEM((16, 8, hidden_size), bf16),
            pltpu.VMEM((16, 8, hidden_size), bf16),
            pltpu.VMEM((16, 8, hidden_size), bf16),
            pltpu.VMEM((8, hidden_size), f32),
            pltpu.VMEM((8, hidden_size), bf16),
            pltpu.VMEM((8, 8, hidden_size), bf16),
            pltpu.VMEM((16, 8, hidden_size), bf16),
            pltpu.VMEM((16, 8, hidden_size), bf16),
            pltpu.VMEM((1, hidden_size), f32),
            pltpu.VMEM((1, hidden_size), f32),
            pltpu.VMEM((1, hidden_size), f32),
            pltpu.VMEM((16, 1, hidden_size), f32),
            pltpu.VMEM((1, hidden_size), f32),
            pltpu.VMEM((8, 1, hidden_size), f32),
            dma((9,)),
        ] + [dma((peers,)) for _ in range(6)] + [
            dma((2,)), dma((16,)), dma((16,)), dma((8,)), dma((8,)),
            dma((16,)), dma((16,)), dma((16,)), dma((16,)),
            dma((2,)), dma((16,)), dma((16,)), dma((8,)), dma((8,)),
        ],
        compiler_params=pltpu.CompilerParams(collective_id=0, has_side_effects=True, vmem_limit_bytes=60 << 20),
        name="step",
    )(
        slot_table,
        slot_table.reshape(1, tables),
        sample_ids.reshape(count, columns),
        id_weights.reshape(count, columns),
        dense_features.reshape(count, width),
        table_shards,
        click_labels,
        top_weight,
        top_bias.reshape(1, hidden_size),
        out_weight,
    )
    return logits, grad_top, grad_bias.reshape(hidden_size)


def solution(mesh):
    return jax.shard_map(
        per_device,
        mesh=mesh,
        in_specs=(
            P(None, ("grp", "tab"), None),
            P(None, ("grp", "tab"), None),
            P(None, ("grp", "tab"), None),
            P(None, ("grp", "tab")),
            P("tab", None, None),
            P(),
            P(),
            P(),
            P(),
        ),
        out_specs=(P(None, ("grp", "tab")), P(), P()),
        check_vma=False,
    )
```
